32 devices in a mesh: rep: 8 (over y, x, core), fsdp: 4 (over z).
Axes of the slice: x: 2, y: 2, z: 4, core: 2. Of those that a mesh axis runs over, the one named last changes fastest.
Arguments:
- tokens: bfloat16 [16384, 768], P(('rep', 'fsdp')), may hold values from -6 to 6
- cotangent: bfloat16 [16384, 768], P(('rep', 'fsdp')), may hold values from -6 to 6
- lengths: int32 [32], P(('rep', 'fsdp')), may hold values from 1 to 512, 10240 in all
- slot_seq: int32 [32], replicated, may hold values from 0 to 31, each once
- query_weight: bfloat16 [768, 768], P('fsdp'), may hold values from -0.21875 to 0.21875
- query_bias: bfloat16 [768], P('fsdp'), may hold values from -2 to 2
- key_weight: bfloat16 [768, 768], P('fsdp'), may hold values from -0.21875 to 0.21875
- value_weight: bfloat16 [768, 768], P('fsdp'), may hold values from -0.21875 to 0.21875
- value_bias: bfloat16 [768], P('fsdp'), may hold values from -2 to 2
- out_weight: bfloat16 [768, 768], P('fsdp'), may hold values from -2.5 to 2.5
- out_bias: bfloat16 [768], P('fsdp'), may hold values from -2 to 2
- first_gain: bfloat16 [768], P('fsdp'), may hold values from 0.5 to 1.5
- first_shift: bfloat16 [768], P('fsdp'), may hold values from -2 to 2
- inner_weight: bfloat16 [768, 3072], P('fsdp'), may hold values from -0.21875 to 0.21875
- inner_bias: bfloat16 [3072], P('fsdp'), may hold values from -2 to 2
- outer_weight: bfloat16 [3072, 768], P('fsdp'), may hold values from -0.109375 to 0.109375
- outer_bias: bfloat16 [768], P('fsdp'), may hold values from -2 to 2
- second_gain: bfloat16 [768], P('fsdp'), may hold values from 0.5 to 1.5
- second_shift: bfloat16 [768], P('fsdp'), may hold values from -2 to 2
Outputs:
- output: bfloat16 [16384, 768], P(('rep', 'fsdp'))
- grad_tokens: bfloat16 [16384, 768], P(('rep', 'fsdp'))
- query_weight_grad: float32 [768, 768], P('fsdp')
- query_bias_grad: float32 [768], P('fsdp')
- key_weight_grad: float32 [768, 768], P('fsdp')
- value_weight_grad: float32 [768, 768], P('fsdp')
- value_bias_grad: float32 [768], P('fsdp')
- out_weight_grad: float32 [768, 768], P('fsdp')
- out_bias_grad: float32 [768], P('fsdp')
- first_gain_grad: float32 [768], P('fsdp')
- first_shift_grad: float32 [768], P('fsdp')
- inner_weight_grad: float32 [768, 3072], P('fsdp')
- inner_bias_grad: float32 [3072], P('fsdp')
- outer_weight_grad: float32 [3072, 768], P('fsdp')
- outer_bias_grad: float32 [768], P('fsdp')
- second_gain_grad: float32 [768], P('fsdp')
- second_shift_grad: float32 [768], P('fsdp')
The draws below stay inside these ranges and needn't reach their ends.
Inputs may be any that keep to these rules, and one draw needn't show every extreme that they name: Every sequence has at least one token; the longest has exactly 512; the lengths add up to 10240. `slot_seq`: each sequence fills exactly one slot.
All inputs are finite; a program needn't handle non-finite values. No bound on the sum of `lengths` on one device may be relied on, other than what follows from the above.
Results may differ from the reference program's by a relative error of at most 0.017.
Values may be sent and summed in bfloat16 or wider, within the bound.
A program may use at most 128 MiB of HBM per device.

```python
import math
import jax
import jax.numpy as jnp
import numpy as np
from jax import lax

D = 768
HEADS = 12
FF = 3072
HD = 64
LMAX = 512
SEQS = 32
TOKENS = 16384
BLOCK = 16
VALID = 10240


def steps_of(key, shape, shards, least, high):
    loudness = 1.0
    for dim, blocks in shards:
        draws = jax.random.uniform(jax.random.fold_in(jax.random.fold_in(key, 6), dim), (blocks,), jnp.float32, least / len(shards), high / len(shards))
        loudness = loudness * jnp.repeat(jnp.exp(draws), shape[dim] // blocks).reshape((-1,) + (1,) * (len(shape) - 1 - dim))
    return loudness


def profile(amount, total, reach, skew):
    portions = [(1 << 20) // math.isqrt(grade ** skew) + 1 for grade in range(2, amount + 1)]
    rest, given = total - reach - (amount - 1), [1] * (amount - 1)
    while rest > 0:
        free = [i for i in range(amount - 1) if given[i] < reach]
        pool, remaining = sum([portions[i] for i in free]), rest
        for i in free:
            addition = min(reach - given[i], max(1, remaining * portions[i] // pool), rest)
            given[i] = given[i] + addition
            rest = rest - addition
    return np.array([reach] + given)


def uneven(rng, amount, total, reach, lean):
    if amount == 2:
        one = jax.random.randint(rng, (), max(1, total - reach), min(reach, total - 1) + 1)
        return jnp.stack([one, total - one])
    sizes = jnp.asarray(profile(amount, total, reach, lean), jnp.int32)
    twos = (amount - 1) // 2
    giver, receiver = sizes[1:1 + 2 * twos:2], sizes[2:2 + 2 * twos:2]
    margin = jnp.minimum(giver - 1, reach - receiver)
    moved = jax.random.randint(jax.random.fold_in(rng, 1), (twos,), 0, 1 << 20) % (margin + 1)
    sizes = sizes.at[1:1 + 2 * twos:2].set(giver - moved).at[2:2 + 2 * twos:2].set(receiver + moved)
    return sizes[jax.random.permutation(jax.random.fold_in(rng, 2), amount)]


def normal_values(own_key, extent, scale, bound, split=(), kind=jnp.bfloat16):
    values = scale * jax.random.normal(own_key, extent, jnp.float32)
    if split:
        values = values * steps_of(own_key, extent, split, -0.22, 0.18)
    return jnp.clip(values, -bound, bound).astype(kind)


def setup_inputs(seed: int = 0) -> dict:
    splits = jax.random.split(jax.random.key(seed), 20)
    return {
        "tokens": normal_values(splits[0], (TOKENS, D), 1.0, 6.0, ((0, 32),)),
        "cotangent": normal_values(splits[1], (TOKENS, D), 1.0, 6.0, ((0, 32),)),
        "lengths": uneven(splits[2], SEQS, VALID, LMAX, 2).astype(jnp.int32),
        "slot_seq": jax.random.permutation(splits[3], SEQS).astype(jnp.int32),
        "query_weight": normal_values(splits[4], (D, D), D ** -0.5, 0.21875, ((0, 4),)),
        "query_bias": normal_values(splits[5], (D,), 0.3, 2.0, ((0, 4),)),
        "key_weight": normal_values(splits[6], (D, D), D ** -0.5, 0.21875, ((0, 4),)),
        "value_weight": normal_values(splits[7], (D, D), D ** -0.5, 0.21875, ((0, 4),)),
        "value_bias": normal_values(splits[8], (D,), 0.3, 2.0, ((0, 4),)),
        "out_weight": normal_values(splits[9], (D, D), (max(1, 4 * D // LMAX)) ** -0.5, 2.5, ((0, 4),)),
        "out_bias": normal_values(splits[10], (D,), 0.3, 2.0, ((0, 4),)),
        "first_gain": jnp.clip(1.0 + 0.1 * jax.random.normal(splits[11], (D,), jnp.float32), 0.5, 1.5).astype(jnp.bfloat16),
        "first_shift": normal_values(splits[12], (D,), 0.3, 2.0, ((0, 4),)),
        "inner_weight": normal_values(splits[13], (D, FF), D ** -0.5, 0.21875, ((0, 4),)),
        "inner_bias": normal_values(splits[14], (FF,), 0.3, 2.0, ((0, 4),)),
        "outer_weight": normal_values(splits[15], (FF, D), FF ** -0.5, 0.109375, ((0, 4),)),
        "outer_bias": normal_values(splits[16], (D,), 0.3, 2.0, ((0, 4),)),
        "second_gain": jnp.clip(1.0 + 0.1 * jax.random.normal(splits[17], (D,), jnp.float32), 0.5, 1.5).astype(jnp.bfloat16),
        "second_shift": normal_values(splits[18], (D,), 0.3, 2.0, ((0, 4),)),
    }


@jax.custom_vjp
def low(v):
    return lax.optimization_barrier(v.astype(jnp.bfloat16)).astype(jnp.float32)

@jax.custom_vjp
def low_back(v):
    return v

def low_keep(v):
    return (low(v), None)

def low_pass(kept, grad):
    return (grad,)

def back_keep(v):
    return (v, None)

def back_low(kept, grad):
    return (low(grad),)
low.defvjp(low_keep, low_pass)
low_back.defvjp(back_keep, back_low)
norm_eps = 1e-12
masked_score = -1e+30

def product(left, right):
    return jnp.dot(left, right, precision=lax.Precision.HIGHEST, preferred_element_type=jnp.float32)

def layer_norm(values, norm_gain, norm_shift):
    center = values - lax.optimization_barrier(jnp.mean(values, axis=-1, keepdims=True))
    spread = lax.optimization_barrier(jnp.mean(center * center, axis=-1, keepdims=True))
    return center * lax.rsqrt(spread + norm_eps) * norm_gain + norm_shift

def attend(inputs):
    queries, key_rows, value_rows, kept_keys = inputs
    scores = jnp.einsum('hqd,hkd->hqk', queries, key_rows, precision=lax.Precision.HIGHEST) * HD ** (-0.5)
    scores = low_back(scores)
    scores = jnp.where(kept_keys[None, None, :], scores, masked_score)
    largest = lax.optimization_barrier(jnp.max(scores, axis=-1, keepdims=True))
    weights = jnp.exp(scores - largest)
    softmax_rows = weights / lax.optimization_barrier(jnp.sum(weights, axis=-1, keepdims=True))
    return jnp.einsum('hqk,hkd->hqd', low(softmax_rows), value_rows, precision=lax.Precision.HIGHEST)

def layer(sequences, params, kept_rows):
    query_weight, query_bias, key_weight, value_weight, value_bias, out_weight, out_bias, first_gain, first_shift, inner_weight, inner_bias, outer_weight, outer_bias, second_gain, second_shift = params
    packed = sequences.shape[0]
    flat_rows = sequences.reshape(packed * LMAX, D)
    queries = low(low_back(product(flat_rows, query_weight) + query_bias))
    key_rows = low(low_back(product(flat_rows, key_weight)))
    value_rows = low(low_back(product(flat_rows, value_weight) + value_bias))

    def split_heads(matrix):
        return matrix.reshape(packed, LMAX, HEADS, HD).transpose(0, 2, 1, 3)
    context = lax.map(jax.checkpoint(attend), (split_heads(queries), split_heads(key_rows), split_heads(value_rows), kept_rows))
    context = context.transpose(0, 2, 1, 3).reshape(packed * LMAX, D)
    context = low(low_back(context))
    attended = low_back(product(context, out_weight) + out_bias)
    hidden = layer_norm(flat_rows + attended, first_gain, first_shift)
    inner = low_back(product(low(hidden), inner_weight) + inner_bias)
    activated = low(jax.nn.gelu(inner, approximate=False))
    outer = low_back(product(activated, outer_weight) + outer_bias)
    result = layer_norm(hidden + outer, second_gain, second_shift)
    result = jnp.where(kept_rows.reshape(-1, 1), result, 0.0)
    return result.reshape(packed, LMAX, D)

def reference(tokens, cotangent, lengths, slot_seq, query_weight, query_bias, key_weight, value_weight, value_bias, out_weight, out_bias, first_gain, first_shift, inner_weight, inner_bias, outer_weight, outer_bias, second_gain, second_shift):
    inverse = jnp.zeros((SEQS,), jnp.int32).at[slot_seq].set(jnp.arange(SEQS, dtype=jnp.int32))

    def to_sequences(array):
        blocks = array.reshape(SEQS, SEQS, BLOCK, D)[:, inverse]
        return blocks.transpose(1, 0, 2, 3).reshape(SEQS, LMAX, D).astype(jnp.float32)

    def to_slots(array):
        blocks = array.reshape(SEQS, SEQS, BLOCK, D).transpose(1, 0, 2, 3)[:, slot_seq]
        return blocks.reshape(TOKENS, D)
    inputs = to_sequences(tokens)
    seeds = to_sequences(cotangent)
    params = tuple((weight.astype(jnp.float32) for weight in (query_weight, query_bias, key_weight, value_weight, value_bias, out_weight, out_bias, first_gain, first_shift, inner_weight, inner_bias, outer_weight, outer_bias, second_gain, second_shift)))
    kept_rows = jnp.arange(LMAX, dtype=jnp.int32)[None, :] < lengths[:, None]
    packed = 1
    while packed * 2 * LMAX <= 4096 and SEQS % (packed * 2) == 0:
        packed = packed * 2
    groups = SEQS // packed

    def one_group(totals, item):
        group_in, group_seed, group_kept = item
        result, backward = jax.vjp(lambda rows_in, weights_in: layer(rows_in, weights_in, group_kept), group_in, params)
        grad_rows, grad_params = backward(group_seed)
        totals = tuple((left + right for left, right in zip(totals, grad_params)))
        return (totals, (result.astype(jnp.bfloat16), grad_rows.astype(jnp.bfloat16)))
    zeros = tuple((jnp.zeros_like(weight) for weight in params))
    totals, (outputs, grad_rows) = lax.scan(one_group, zeros, (inputs.reshape(groups, packed, LMAX, D), seeds.reshape(groups, packed, LMAX, D), kept_rows.reshape(groups, packed, LMAX)))
    output = to_slots(outputs.reshape(SEQS, LMAX, D))
    grad_tokens = to_slots(grad_rows.reshape(SEQS, LMAX, D))
    return (output, grad_tokens, totals[0], totals[1], totals[2], totals[3], totals[4], totals[5], totals[6], totals[7], totals[8], totals[9], totals[10], totals[11], totals[12], totals[13], totals[14])
```

```python
import functools
import math

import jax
import jax.numpy as jnp
from jax import lax
from jax.experimental import pallas as pl
from jax.experimental.pallas import tpu as pltpu
from jax.sharding import PartitionSpec as P

HEADS = 12
HD = 64
MESH = pl.DeviceIdType.MESH
DMA = pltpu.SemaphoreType.DMA
QUAD = 4


norm_eps = 1e-12
masked_score = -1e30
inv_root_two = 0.7071067811865476
inv_root_two_pi = 0.3989422804014327


def remote(src, dst, send, recv, device):
    return pltpu.make_async_remote_copy(
        src_ref=src, dst_ref=dst, send_sem=send, recv_sem=recv,
        device_id=device, device_id_type=MESH,
    )


def place(linear, fsdp_size):
    return {"rep": lax.div(linear, fsdp_size), "fsdp": lax.rem(linear, fsdp_size)}


def enter(count, fsdp_size, me):
    sem = pltpu.get_barrier_semaphore()

    def greet(k, carry):
        pl.semaphore_signal(
            sem, inc=1, device_id=place(lax.rem(me + k, count), fsdp_size), device_id_type=MESH
        )
        return carry

    lax.fori_loop(1, count, greet, 0)
    pl.semaphore_wait(sem, count - 1)


class Exchange:
    def __init__(self, count, fsdp_size, me, src, dst, rows, sems, spread=False):
        self.args = (count, fsdp_size, me, src, dst, rows, sems, spread)

    def copy(self, k, arriving):
        count, fsdp_size, me, src, dst, rows, (send, recv), spread = self.args
        peer = lax.rem(me + k, count)
        slot = lax.rem(me + count - k, count) if arriving else me
        source = src if spread else src.at[pl.ds(pl.multiple_of(peer * rows, rows), rows)]
        return remote(
            source, dst.at[pl.ds(pl.multiple_of(slot * rows, rows), rows)],
            send.at[k], recv.at[k], place(peer, fsdp_size),
        )

    def start(self):
        def go(k, carry):
            self.copy(k, False).start()
            return carry

        lax.fori_loop(1, self.args[0], go, 0)

    def wait(self):
        def go(k, carry):
            self.copy(k, True).wait()
            return carry

        lax.fori_loop(1, self.args[0], go, 0)


def block_of(ref, index, rows):
    return ref.at[pl.ds(pl.multiple_of(index * rows, rows), rows)]


def position(fsdp_size):
    r = lax.axis_index("rep")
    f = lax.axis_index("fsdp")
    core = lax.rem(r, 2)
    chip = lax.div(r, 2)
    q = lax.rem(chip, QUAD)
    return r, f, core, chip, q, chip - q


def fetch_kernel(rep_size, fsdp_size, weights, *refs):
    F = fsdp_size
    refs = list(refs)
    take = lambda k: [refs.pop(0) for _ in range(k)]
    tok, cot, length, vec = take(4)
    shard = take(weights)
    otok, ocot, olen, ovec = take(4)
    full = take(weights)
    stage = take(weights)
    xs, xr, ys, yr, ls, lr, vs, vr, zs, zr, qs, qr, ps, pr, own = take(15)
    r, f, core, chip, q, base = position(F)
    count = rep_size * F
    me = r * F + f
    rows = tok.shape[0] // count
    vrows = vec.shape[0]
    lrows = length.shape[0]
    enter(count, F, me)

    trade_tok = Exchange(count, F, me, tok, otok, rows, (xs, xr))
    trade_cot = Exchange(count, F, me, cot, ocot, rows, (ys, yr))
    trade_len = Exchange(count, F, me, length, olen, lrows, (ls, lr), spread=True)

    def piece(ref, w, shard_row, quarter):
        S, C = shard[w].shape
        sq, half = S // QUAD, C // 2
        return ref.at[
            pl.ds(pl.multiple_of(shard_row * S + quarter * sq, sq), sq),
            pl.ds(pl.multiple_of(core * half, half), half),
        ]

    def strip(w, shard_row, which):
        S, C = shard[w].shape
        half = C // 2
        return full[w].at[
            pl.ds(pl.multiple_of(shard_row * S, S), S), pl.ds(pl.multiple_of(which * half, half), half)
        ]

    def mate(m):
        return {"rep": (base + lax.rem(q + m, QUAD)) * 2 + core, "fsdp": f}

    partner = {"rep": chip * 2 + (1 - core), "fsdp": f}

    def along(w, j, arriving):
        to = lax.rem(f + j, F)
        row = lax.rem(f + F - j, F) if arriving else f
        return remote(
            piece(shard[w], w, 0, q), piece(full[w], w, row, q),
            zs.at[w, j], zr.at[w, j], {"rep": r, "fsdp": to},
        )

    def across(w, j, m, arriving):
        row = lax.rem(f + F - j, F)
        part = piece(full[w], w, row, lax.rem(q + QUAD - m, QUAD) if arriving else q)
        return remote(part, part, qs.at[w, j, m], qr.at[w, j, m], mate(m))

    def beside(w, j, arriving):
        row = lax.rem(f + F - j, F)
        part = strip(w, row, (1 - core) if arriving else core)
        return remote(part, part, ps.at[w, j], pr.at[w, j], partner)

    def vector(j, arriving):
        to = lax.rem(f + j, F)
        row = lax.rem(f + F - j, F) if arriving else f
        return remote(vec, block_of(ovec, row, vrows), vs.at[j], vr.at[j], {"rep": r, "fsdp": to})

    trade_len.start()
    for j in range(1, F):
        vector(j, False).start()
    trade_tok.start()
    for w in range(weights):
        for j in range(1, F):
            along(w, j, False).start()
    trade_cot.start()

    local = [
        pltpu.make_async_copy(block_of(tok, me, rows), block_of(otok, me, rows), own.at[0]),
        pltpu.make_async_copy(block_of(cot, me, rows), block_of(ocot, me, rows), own.at[1]),
        pltpu.make_async_copy(length, block_of(olen, me, lrows), own.at[2]),
        pltpu.make_async_copy(vec, block_of(ovec, f, vrows), own.at[3]),
    ]
    into = [pltpu.make_async_copy(shard[w], stage[w], own.at[4 + w]) for w in range(weights)]
    for c in local + into:
        c.start()
    out = []
    for w in range(weights):
        into[w].wait()
        c = pltpu.make_async_copy(stage[w], block_of(full[w], f, shard[w].shape[0]), own.at[4 + w])
        c.start()
        out.append(c)

    def step_two(w):
        for j in range(1, F):
            along(w, j, True).wait_recv()
            for m in range(1, QUAD):
                across(w, j, m, False).start()

    def step_three(w):
        for j in range(1, F):
            for m in range(1, QUAD):
                across(w, j, m, True).wait_recv()
            beside(w, j, False).start()

    def step_four(w):
        for j in range(1, F):
            beside(w, j, True).wait_recv()

    for w in range(weights + 2):
        if w < weights:
            step_two(w)
        if 0 <= w - 1 < weights:
            step_three(w - 1)
        if 0 <= w - 2 < weights:
            step_four(w - 2)
    for w in range(weights):
        for j in range(1, F):
            along(w, j, False).wait_send()
            for m in range(1, QUAD):
                across(w, j, m, False).wait_send()
            beside(w, j, False).wait_send()
    for j in range(1, F):
        vector(j, True).wait()
    for c in local + out:
        c.wait()
    trade_len.wait()
    trade_tok.wait()
    trade_cot.wait()


def fetch(rep_size, fsdp_size, tok, cot, length, vec, shards_in):
    weights = len(shards_in)
    count = rep_size * fsdp_size
    F = fsdp_size
    like = jax.ShapeDtypeStruct
    outs = [
        like(tok.shape, tok.dtype), like(cot.shape, cot.dtype),
        like((count * length.shape[0], length.shape[1]), length.dtype),
        like((F * vec.shape[0], vec.shape[1]), vec.dtype),
    ] + [like((w.shape[0] * F, w.shape[1]), w.dtype) for w in shards_in]
    anywhere = pl.BlockSpec(memory_space=pl.ANY)
    return pl.pallas_call(
        functools.partial(fetch_kernel, rep_size, fsdp_size, weights),
        out_shape=outs,
        in_specs=[anywhere] * (4 + weights),
        out_specs=[anywhere] * (4 + weights),
        scratch_shapes=[pltpu.VMEM(w.shape, w.dtype) for w in shards_in]
        + [DMA((count,))] * 6
        + [DMA((F,))] * 2
        + [DMA((weights, F))] * 2
        + [DMA((weights, F, QUAD))] * 2
        + [DMA((weights, F))] * 2
        + [DMA((4 + weights,))],
        compiler_params=pltpu.CompilerParams(collective_id=1, has_side_effects=True),
        name="fetch",
    )(tok, cot, length, vec, *shards_in)


def add_into(dst, left, parts, rows):
    def go(i, carry):
        at = pl.ds(pl.multiple_of(i * rows, rows), rows)
        total = left[at, :].astype(jnp.float32)
        for part in parts:
            total = total + part[at, :].astype(jnp.float32)
        dst[at, :] = total.astype(dst.dtype)
        return carry

    lax.fori_loop(0, dst.shape[0] // rows, go, 0)


def reduce_kernel(rep_size, fsdp_size, weights, *refs):
    F = fsdp_size
    refs = list(refs)
    take = lambda k: [refs.pop(0) for _ in range(k)]
    res, gin = take(2)
    grads = take(weights)
    ores, ogin = take(2)
    owned = take(weights)
    half_in = take(weights)
    half_own = take(weights)
    quad_in = take(weights)
    quad_sum = take(weights)
    line_in = take(weights)
    line_sum = take(weights)
    group_count = rep_size // (2 * QUAD)
    group_in = take(weights) if group_count > 1 else None
    xs, xr, ys, yr, ps, pr, qs, qr, zs, zr, gs, gr, hs, hr, bs, br, own = take(17)
    r, f, core, chip, q, base = position(F)
    count = rep_size * F
    me = r * F + f
    rows = res.shape[0] // count
    enter(count, F, me)

    trade_res = Exchange(count, F, me, res, ores, rows, (xs, xr))
    trade_gin = Exchange(count, F, me, gin, ogin, rows, (ys, yr))
    partner = {"rep": chip * 2 + (1 - core), "fsdp": f}

    def mate(m):
        return {"rep": (base + lax.rem(q + m, QUAD)) * 2 + core, "fsdp": f}

    def columns(ref, w, which):
        half = grads[w].shape[1] // 2
        return ref.at[:, pl.ds(pl.multiple_of(which * half, half), half)]

    def swap(w):
        return remote(columns(grads[w], w, 1 - core), half_in[w], ps.at[w], pr.at[w], partner)

    def size(w):
        S = grads[w].shape[0] // F
        return S, S // QUAD

    def across(w, m, t):
        S, sq = size(w)
        goal = lax.rem(q + m, QUAD)
        return remote(
            half_in[w].at[pl.ds(pl.multiple_of(t * S + goal * sq, sq), sq)],
            quad_in[w].at[m - 1, pl.ds(t * sq, sq)],
            qs.at[w, m, t], qr.at[w, m, t], mate(m),
        )

    def along(w, j):
        S, sq = size(w)
        to = lax.rem(f + j, F)
        return remote(
            quad_sum[w].at[pl.ds(pl.multiple_of(to * sq, sq), sq)], line_in[w].at[j - 1],
            zs.at[w, j], zr.at[w, j], {"rep": r, "fsdp": to},
        )

    def group(w, g):
        to = lax.rem(lax.div(chip, QUAD) + g, group_count)
        return remote(
            line_sum[w], group_in[w].at[g - 1], gs.at[w, g], gr.at[w, g],
            {"rep": (to * QUAD + q) * 2 + core, "fsdp": f},
        )

    def home(w, quarter, which):
        S, sq = size(w)
        half = grads[w].shape[1] // 2
        return owned[w].at[
            pl.ds(pl.multiple_of(quarter * sq, sq), sq), pl.ds(pl.multiple_of(which * half, half), half)
        ]

    def spread(w, m, arriving):
        S, sq = size(w)
        return remote(
            line_sum[w], home(w, lax.rem(q + QUAD - m, QUAD) if arriving else q, core),
            hs.at[w, m], hr.at[w, m], mate(m),
        )

    def beside(w, arriving):
        part = columns(owned[w], w, (1 - core) if arriving else core)
        return remote(part, part, bs.at[w], br.at[w], partner)

    for w in range(weights):
        swap(w).start()
    local = [
        pltpu.make_async_copy(block_of(res, me, rows), block_of(ores, me, rows), own.at[0]),
        pltpu.make_async_copy(block_of(gin, me, rows), block_of(ogin, me, rows), own.at[1]),
    ]
    kept = [
        pltpu.make_async_copy(columns(grads[w], w, core), half_own[w], own.at[2 + w])
        for w in range(weights)
    ]
    for c in local + kept:
        c.start()

    def step_one(w):
        kept[w].wait()
        swap(w).wait_recv()
        add_into(half_in[w], half_in[w], [half_own[w]], size(w)[1])
        for m in range(1, QUAD):
            for t in range(F):
                across(w, m, t).start()

    def step_two(w):
        S, sq = size(w)
        for m in range(1, QUAD):
            for t in range(F):
                across(w, m, t).wait_recv()

        def go(t, carry):
            at = pl.ds(pl.multiple_of(t * sq, sq), sq)
            total = half_in[w][pl.ds(pl.multiple_of(t * S + q * sq, sq), sq), :].astype(jnp.float32)
            for m in range(QUAD - 1):
                total = total + quad_in[w][m, at, :].astype(jnp.float32)
            quad_sum[w][at, :] = total.astype(quad_sum[w].dtype)
            return carry

        lax.fori_loop(0, F, go, 0)
        for j in range(1, F):
            along(w, j).start()

    def step_three(w):
        S, sq = size(w)
        for j in range(1, F):
            along(w, j).wait_recv()
        total = quad_sum[w][pl.ds(pl.multiple_of(f * sq, sq), sq), :].astype(jnp.float32)
        for j in range(F - 1):
            total = total + line_in[w][j].astype(jnp.float32)
        line_sum[w][...] = total.astype(line_sum[w].dtype)
        for g in range(1, group_count):
            group(w, g).start()
        if group_count == 1:
            finish(w)

    def step_group(w):
        for g in range(1, group_count):
            group(w, g).wait()
        total = line_sum[w][...].astype(jnp.float32)
        for g in range(group_count - 1):
            total = total + group_in[w][g].astype(jnp.float32)
        line_sum[w][...] = total.astype(line_sum[w].dtype)
        finish(w)

    def finish(w):
        for m in range(1, QUAD):
            spread(w, m, False).start()
        c = pltpu.make_async_copy(line_sum[w], home(w, q, core), own.at[2 + w])
        c.start()
        c.wait()

    def step_four(w):
        for m in range(1, QUAD):
            spread(w, m, True).wait_recv()
        beside(w, False).start()

    steps = [step_one, step_two, step_three] + ([step_group] if group_count > 1 else []) + [step_four]
    for at in range(weights + len(steps) - 1):
        for k, step in enumerate(steps):
            if 0 <= at - k < weights:
                step(at - k)
        if at == 0:
            trade_res.start()
            trade_gin.start()
    for w in range(weights):
        beside(w, True).wait_recv()
        swap(w).wait_send()
        for m in range(1, QUAD):
            for t in range(F):
                across(w, m, t).wait_send()
            spread(w, m, False).wait_send()
        for j in range(1, F):
            along(w, j).wait_send()
        beside(w, False).wait_send()
    for c in local:
        c.wait()
    trade_res.wait()
    trade_gin.wait()


def reduce_all(rep_size, fsdp_size, res, gin, grads):
    weights = len(grads)
    count = rep_size * fsdp_size
    F = fsdp_size
    groups = rep_size // (2 * QUAD)
    like = jax.ShapeDtypeStruct
    anywhere = pl.BlockSpec(memory_space=pl.ANY)
    outs = [like(res.shape, res.dtype), like(gin.shape, gin.dtype)] + [
        like((g.shape[0] // F, g.shape[1]), g.dtype) for g in grads
    ]
    V = pltpu.VMEM
    scratch = [V((g.shape[0], g.shape[1] // 2), g.dtype) for g in grads]
    scratch += [V((g.shape[0], g.shape[1] // 2), g.dtype) for g in grads]
    scratch += [V((QUAD - 1, g.shape[0] // QUAD, g.shape[1] // 2), g.dtype) for g in grads]
    scratch += [V((g.shape[0] // QUAD, g.shape[1] // 2), g.dtype) for g in grads]
    scratch += [V((F - 1, g.shape[0] // QUAD // F, g.shape[1] // 2), g.dtype) for g in grads]
    scratch += [V((g.shape[0] // QUAD // F, g.shape[1] // 2), g.dtype) for g in grads]
    if groups > 1:
        scratch += [V((groups - 1, g.shape[0] // QUAD // F, g.shape[1] // 2), g.dtype) for g in grads]
    scratch += [DMA((count,))] * 4 + [DMA((weights,))] * 2 + [DMA((weights, QUAD, F))] * 2
    scratch += [DMA((weights, F))] * 2 + [DMA((weights, max(groups, 2)))] * 2
    scratch += [DMA((weights, QUAD))] * 2 + [DMA((weights,))] * 2 + [DMA((2 + weights,))]
    return pl.pallas_call(
        functools.partial(reduce_kernel, rep_size, fsdp_size, weights),
        out_shape=outs,
        in_specs=[anywhere] * (2 + weights),
        out_specs=[anywhere] * (2 + weights),
        scratch_shapes=scratch,
        compiler_params=pltpu.CompilerParams(
            collective_id=2, has_side_effects=True, vmem_limit_bytes=56 * 2**20
        ),
        name="reduce_all",
    )(res, gin, *grads)


def matmul(left, right):
    return jnp.dot(left, right, preferred_element_type=jnp.float32)


def matmul_left_t(left, right):
    return lax.dot_general(
        left, right, (((0,), (0,)), ((), ())), preferred_element_type=jnp.float32
    )


def matmul_right_t(left, right):
    return lax.dot_general(
        left, right, (((1,), (1,)), ((), ())), preferred_element_type=jnp.float32
    )


def norm_forward(values, norm_gain, norm_shift):
    center = values - jnp.mean(values, axis=-1, keepdims=True)
    spread = jnp.mean(center * center, axis=-1, keepdims=True)
    scaled_inv = lax.rsqrt(spread + norm_eps)
    normed = center * scaled_inv
    return (normed * norm_gain + norm_shift, normed, scaled_inv)


def norm_backward(grad_out, normed, scaled_inv, norm_gain):
    grad_normed = grad_out * norm_gain
    first_mean = jnp.mean(grad_normed, axis=-1, keepdims=True)
    second_mean = jnp.mean(grad_normed * normed, axis=-1, keepdims=True)
    return (grad_normed - first_mean - normed * second_mean) * scaled_inv


def score_block(query_block, key_rows, kept_keys):
    scores = jnp.einsum(
        "qhd,khd->hqk", query_block, key_rows, preferred_element_type=jnp.float32
    ) * HD ** (-0.5)
    return jnp.where(kept_keys[None, None, :], scores, masked_score)


def attention_forward(query_rows, key_rows, value_rows, kept_keys, block_rows):
    seq_len = query_rows.shape[0]

    def one_block(query_block):
        scores = score_block(query_block, key_rows, kept_keys)
        largest = jnp.max(scores, axis=-1, keepdims=True)
        weights = jnp.exp(scores - largest)
        row_total = jnp.sum(weights, axis=-1, keepdims=True)
        chances = (weights / row_total).astype(jnp.bfloat16)
        context = jnp.einsum(
            "hqk,khd->qhd", chances, value_rows, preferred_element_type=jnp.float32
        )
        return (context, largest + jnp.log(row_total))

    blocks = query_rows.reshape(seq_len // block_rows, block_rows, HEADS, HD)
    context, log_total = lax.map(one_block, blocks)
    return (context.reshape(seq_len, HEADS * HD), log_total)


def attention_backward(
    query_rows, key_rows, value_rows, kept_keys, grad_context, log_total, block_rows
):
    seq_len = query_rows.shape[0]
    block_count = seq_len // block_rows
    scale = HD ** (-0.5)

    def one_block(carry, item):
        grad_keys, grad_values = carry
        query_block, grad_block, log_block = item
        scores = score_block(query_block, key_rows, kept_keys)
        chances = jnp.exp(scores - log_block)
        grad_chances = jnp.einsum(
            "qhd,khd->hqk", grad_block, value_rows, preferred_element_type=jnp.float32
        )
        centered = jnp.sum(chances * grad_chances, axis=-1, keepdims=True)
        grad_scores = (chances * (grad_chances - centered)).astype(jnp.bfloat16)
        grad_query = (
            jnp.einsum("hqk,khd->qhd", grad_scores, key_rows, preferred_element_type=jnp.float32)
            * scale
        )
        grad_keys = (
            grad_keys
            + jnp.einsum(
                "hqk,qhd->khd", grad_scores, query_block, preferred_element_type=jnp.float32
            )
            * scale
        )
        grad_values = grad_values + jnp.einsum(
            "hqk,qhd->khd",
            chances.astype(jnp.bfloat16),
            grad_block,
            preferred_element_type=jnp.float32,
        )
        return ((grad_keys, grad_values), grad_query)

    start = jnp.zeros(key_rows.shape, jnp.float32)
    items = (
        query_rows.reshape(block_count, block_rows, HEADS, HD),
        grad_context.reshape(block_count, block_rows, HEADS, HD),
        log_total,
    )
    (grad_keys, grad_values), grad_query = lax.scan(one_block, (start, start), items)
    return (
        grad_query.reshape(seq_len, HEADS * HD),
        grad_keys.reshape(seq_len, HEADS * HD),
        grad_values.reshape(seq_len, HEADS * HD),
    )


def shards(
    tokens,
    cotangent,
    lengths,
    slot_seq,
    query_weight,
    query_bias,
    key_weight,
    value_weight,
    value_bias,
    out_weight,
    out_bias,
    first_gain,
    first_shift,
    inner_weight,
    inner_bias,
    outer_weight,
    outer_bias,
    second_gain,
    second_shift,
):
    rep_size, fsdp_size = lax.axis_size("rep"), lax.axis_size("fsdp")
    me = lax.axis_index("rep") * fsdp_size + lax.axis_index("fsdp")
    row_count, feature_dim = tokens.shape
    small = [query_bias, value_bias, out_bias, first_gain, first_shift, outer_bias, second_gain, second_shift]
    width = query_bias.shape[0]
    wide = inner_bias.shape[0] // width
    lanes = 256
    vec_rows = 16

    def stack(vectors):
        table = jnp.stack([v.reshape(width) for v in vectors])
        return jnp.pad(table, ((0, vec_rows - table.shape[0]), (0, lanes - width)))

    vec = stack(small + list(inner_bias.reshape(wide, width)))
    length_block = jnp.broadcast_to(lengths.reshape(1, 1), (8, 128))
    (
        seq_rows, seq_seed, all_lengths, all_vec,
        query_full, key_full, value_full, out_full, inner_full, outer_full,
    ) = fetch(
        rep_size, fsdp_size, tokens, cotangent, length_block, vec,
        [query_weight, key_weight, value_weight, out_weight, inner_weight, outer_weight],
    )
    my_length = all_lengths.reshape(-1, 8, 128)[slot_seq[me], 0, 0]
    kept = jnp.arange(row_count, dtype=jnp.int32) < my_length
    table = all_vec.reshape(fsdp_size, vec_rows, lanes)[:, :, :width].astype(jnp.float32)
    (
        query_bias_full, value_bias_full, out_bias_full, first_gain_full, first_shift_full,
        outer_bias_full, second_gain_full, second_shift_full,
    ) = [table[:, i].reshape(-1) for i in range(8)]
    inner_bias_full = table[:, 8 : 8 + wide].reshape(-1)
    block_rows = math.gcd(row_count, 512)
    head_shape = (row_count, HEADS, HD)
    query_rows = (
        (matmul(seq_rows, query_full) + query_bias_full).astype(jnp.bfloat16).reshape(head_shape)
    )
    key_rows = matmul(seq_rows, key_full).astype(jnp.bfloat16).reshape(head_shape)
    value_rows = (
        (matmul(seq_rows, value_full) + value_bias_full).astype(jnp.bfloat16).reshape(head_shape)
    )
    context, log_total = attention_forward(query_rows, key_rows, value_rows, kept, block_rows)
    context = context.astype(jnp.bfloat16)
    attended = matmul(context, out_full) + out_bias_full
    hidden, first_normed, first_inv = norm_forward(
        seq_rows.astype(jnp.float32) + attended, first_gain_full, first_shift_full
    )
    hidden_low = hidden.astype(jnp.bfloat16)
    inner = matmul(hidden_low, inner_full) + inner_bias_full
    activated = jax.nn.gelu(inner, approximate=False).astype(jnp.bfloat16)
    outer = matmul(activated, outer_full) + outer_bias_full
    result, second_normed, second_inv = norm_forward(
        hidden + outer, second_gain_full, second_shift_full
    )
    result = jnp.where(kept[:, None], result, 0.0).astype(jnp.bfloat16)
    seed_rows = jnp.where(kept[:, None], seq_seed.astype(jnp.float32), 0.0)
    grad_second_gain = jnp.sum(seed_rows * second_normed, axis=0)
    grad_second_shift = jnp.sum(seed_rows, axis=0)
    grad_second = norm_backward(seed_rows, second_normed, second_inv, second_gain_full)
    grad_outer = grad_second.astype(jnp.bfloat16)
    grad_outer_bias = jnp.sum(grad_outer, axis=0, dtype=jnp.float32)
    grad_outer_weight = matmul_left_t(activated, grad_outer)
    grad_activated = matmul_right_t(grad_outer, outer_full)
    slope = (
        0.5 * (1.0 + lax.erf(inner * inv_root_two))
        + inner * jnp.exp(-0.5 * inner * inner) * inv_root_two_pi
    )
    grad_inner = (grad_activated * slope).astype(jnp.bfloat16)
    grad_inner_bias = jnp.sum(grad_inner, axis=0, dtype=jnp.float32)
    grad_inner_weight = matmul_left_t(hidden_low, grad_inner)
    grad_hidden = grad_second + matmul_right_t(grad_inner, inner_full)
    grad_first_gain = jnp.sum(grad_hidden * first_normed, axis=0)
    grad_first_shift = jnp.sum(grad_hidden, axis=0)
    grad_residual = norm_backward(grad_hidden, first_normed, first_inv, first_gain_full)
    grad_attended = grad_residual.astype(jnp.bfloat16)
    grad_out_bias = jnp.sum(grad_attended, axis=0, dtype=jnp.float32)
    grad_out_weight = matmul_left_t(context, grad_attended)
    grad_context = matmul_right_t(grad_attended, out_full).astype(jnp.bfloat16)
    grad_query, grad_key, grad_value = attention_backward(
        query_rows, key_rows, value_rows, kept, grad_context.reshape(head_shape), log_total, block_rows
    )
    grad_query = grad_query.astype(jnp.bfloat16)
    grad_key = grad_key.astype(jnp.bfloat16)
    grad_value = grad_value.astype(jnp.bfloat16)
    grad_query_bias = jnp.sum(grad_query, axis=0, dtype=jnp.float32)
    grad_value_bias = jnp.sum(grad_value, axis=0, dtype=jnp.float32)
    grad_query_weight = matmul_left_t(seq_rows, grad_query)
    grad_key_weight = matmul_left_t(seq_rows, grad_key)
    grad_value_weight = matmul_left_t(seq_rows, grad_value)
    grad_input = (
        grad_residual
        + matmul_right_t(grad_query, query_full)
        + matmul_right_t(grad_key, key_full)
        + matmul_right_t(grad_value, value_full)
    ).astype(jnp.bfloat16)
    low = lambda g: g.astype(jnp.bfloat16)
    grad_small = [
        grad_query_bias, grad_value_bias, grad_out_bias, grad_first_gain, grad_first_shift,
        grad_outer_bias, grad_second_gain, grad_second_shift,
    ]
    grad_table = jnp.concatenate(
        [
            jnp.stack(grad_small).reshape(8, fsdp_size, width).transpose(1, 0, 2),
            grad_inner_bias.reshape(fsdp_size, wide, width),
        ],
        axis=1,
    )
    grad_rows = 32
    grad_table = jnp.pad(
        grad_table, ((0, 0), (0, grad_rows - 8 - wide), (0, lanes - width))
    ).reshape(fsdp_size * grad_rows, lanes)
    (
        back_rows, back_grads, d_outer, d_inner, d_out, d_query, d_key, d_value, d_vec,
    ) = reduce_all(
        rep_size, fsdp_size, result, grad_input,
        [
            low(grad_outer_weight), low(grad_inner_weight), low(grad_out_weight),
            low(grad_query_weight), low(grad_key_weight), low(grad_value_weight), grad_table,
        ],
    )
    up = lambda g: g.astype(jnp.float32)
    v = d_vec[:, :width]
    return (
        back_rows, back_grads,
        up(d_query), v[0], up(d_key), up(d_value), v[1], up(d_out), v[2], v[3], v[4],
        up(d_inner), v[8 : 8 + wide].reshape(-1), up(d_outer), v[5], v[6], v[7],
    )


def solution(mesh):
    placed = (
        P(("rep", "fsdp"), None),
        P(("rep", "fsdp"), None),
        P(("rep", "fsdp")),
        P(),
        P("fsdp", None),
        P("fsdp"),
        P("fsdp", None),
        P("fsdp", None),
        P("fsdp"),
        P("fsdp", None),
        P("fsdp"),
        P("fsdp"),
        P("fsdp"),
        P("fsdp", None),
        P("fsdp"),
        P("fsdp", None),
        P("fsdp"),
        P("fsdp"),
        P("fsdp"),
    )
    return jax.shard_map(
        shards,
        mesh=mesh,
        in_specs=placed,
        out_specs=(
            P(("rep", "fsdp"), None),
            P(("rep", "fsdp"), None),
            P("fsdp", None),
            P("fsdp"),
            P("fsdp", None),
            P("fsdp", None),
            P("fsdp"),
            P("fsdp", None),
            P("fsdp"),
            P("fsdp"),
            P("fsdp"),
            P("fsdp", None),
            P("fsdp"),
            P("fsdp", None),
            P("fsdp"),
            P("fsdp"),
            P("fsdp"),
        ),
        check_vma=False,
    )
```

```python
import functools
import math

import jax
import jax.numpy as jnp
from jax import lax
from jax.experimental import pallas as pl
from jax.experimental.pallas import tpu as pltpu
from jax.sharding import PartitionSpec as P

HEADS = 12
HD = 64
MESH = pl.DeviceIdType.MESH
DMA = pltpu.SemaphoreType.DMA
QUAD = 4


norm_eps = 1e-12
masked_score = -1e30
inv_root_two = 0.7071067811865476
inv_root_two_pi = 0.3989422804014327


def remote(src, dst, send, recv, device):
    return pltpu.make_async_remote_copy(
        src_ref=src, dst_ref=dst, send_sem=send, recv_sem=recv,
        device_id=device, device_id_type=MESH,
    )


def place(linear, fsdp_size):
    return {"rep": lax.div(linear, fsdp_size), "fsdp": lax.rem(linear, fsdp_size)}


def enter(count, fsdp_size, me):
    sem = pltpu.get_barrier_semaphore()

    def greet(k, carry):
        pl.semaphore_signal(
            sem, inc=1, device_id=place(lax.rem(me + k, count), fsdp_size), device_id_type=MESH
        )
        return carry

    lax.fori_loop(1, count, greet, 0)
    pl.semaphore_wait(sem, count - 1)


class Exchange:
    def __init__(self, count, fsdp_size, me, src, dst, rows, sems, spread=False):
        self.args = (count, fsdp_size, me, src, dst, rows, sems, spread)

    def copy(self, k, arriving):
        count, fsdp_size, me, src, dst, rows, (send, recv), spread = self.args
        peer = lax.rem(me + k, count)
        slot = lax.rem(me + count - k, count) if arriving else me
        source = src if spread else src.at[pl.ds(pl.multiple_of(peer * rows, rows), rows)]
        return remote(
            source, dst.at[pl.ds(pl.multiple_of(slot * rows, rows), rows)],
            send.at[k], recv.at[k], place(peer, fsdp_size),
        )

    def start(self):
        def go(k, carry):
            self.copy(k, False).start()
            return carry

        lax.fori_loop(1, self.args[0], go, 0)

    def wait(self):
        def go(k, carry):
            self.copy(k, True).wait()
            return carry

        lax.fori_loop(1, self.args[0], go, 0)


def block_of(ref, index, rows):
    return ref.at[pl.ds(pl.multiple_of(index * rows, rows), rows)]


def position(fsdp_size):
    r = lax.axis_index("rep")
    f = lax.axis_index("fsdp")
    core = lax.rem(r, 2)
    chip = lax.div(r, 2)
    q = lax.rem(chip, QUAD)
    return r, f, core, chip, q, chip - q


def flip(q, bit):
    return q + bit - 2 * bit * lax.rem(lax.div(q, bit), 2)


def fetch_kernel(rep_size, fsdp_size, weights, *refs):
    F = fsdp_size
    refs = list(refs)
    take = lambda k: [refs.pop(0) for _ in range(k)]
    tok, cot, length, vec = take(4)
    shard = take(weights)
    otok, ocot, olen, ovec = take(4)
    full = take(weights)
    stage = take(weights)
    xs, xr, ys, yr, ls, lr, vs, vr, zs, zr, qs, qr, ps, pr, own = take(15)
    r, f, core, chip, q, base = position(F)
    count = rep_size * F
    me = r * F + f
    rows = tok.shape[0] // count
    vrows = vec.shape[0]
    lrows = length.shape[0]
    enter(count, F, me)

    trade_tok = Exchange(count, F, me, tok, otok, rows, (xs, xr))
    trade_cot = Exchange(count, F, me, cot, ocot, rows, (ys, yr))
    trade_len = Exchange(count, F, me, length, olen, lrows, (ls, lr), spread=True)

    def piece(ref, w, shard_row, quarter):
        S, C = shard[w].shape
        sq, half = S // QUAD, C // 2
        return ref.at[
            pl.ds(pl.multiple_of(shard_row * S + quarter * sq, sq), sq),
            pl.ds(pl.multiple_of(core * half, half), half),
        ]

    def strip(w, shard_row, which):
        S, C = shard[w].shape
        half = C // 2
        return full[w].at[
            pl.ds(pl.multiple_of(shard_row * S, S), S), pl.ds(pl.multiple_of(which * half, half), half)
        ]

    near = (flip(q, 1), flip(q, 2))
    far = flip(near[0], 2)

    def chip_at(quarter):
        return {"rep": (base + quarter) * 2 + core, "fsdp": f}

    partner = {"rep": chip * 2 + (1 - core), "fsdp": f}

    def along(w, row, step):
        source = piece(full[w], w, row, q)
        return remote(
            source, source, zs.at[w, row, (1 - step) // 2], zr.at[w, row], {"rep": r, "fsdp": f + step}
        )

    def first_along(w, step):
        return remote(
            piece(shard[w], w, 0, q), piece(full[w], w, f, q),
            zs.at[w, f, (1 - step) // 2], zr.at[w, f], {"rep": r, "fsdp": f + step},
        )

    def across(w, row, side, arriving):
        part = piece(full[w], w, row, near[side] if arriving else q)
        return remote(part, part, qs.at[w, row, side], qr.at[w, row, side], chip_at(near[side]))

    def relay(w, row, arriving):
        turn = lax.rem(row + w, 2)
        part = piece(full[w], w, row, far if arriving else jnp.where(turn == 0, near[1], near[0]))
        to = chip_at(jnp.where(turn == 0, near[0], near[1]))
        return remote(part, part, qs.at[w, row, 2], qr.at[w, row, 2], to)

    def beside(w, j, arriving):
        row = lax.rem(f + j, F)
        part = strip(w, row, (1 - core) if arriving else core)
        return remote(part, part, ps.at[w, j], pr.at[w, j], partner)

    def vector(j, arriving):
        to = lax.rem(f + j, F)
        row = lax.rem(f + F - j, F) if arriving else f
        return remote(vec, block_of(ovec, row, vrows), vs.at[j], vr.at[j], {"rep": r, "fsdp": to})

    trade_len.start()
    for j in range(1, F):
        vector(j, False).start()
    trade_tok.start()
    for w in range(weights):
        @pl.when(f < F - 1)
        def _():
            first_along(w, 1).start()

        @pl.when(f > 0)
        def _():
            first_along(w, -1).start()

    trade_cot.start()

    local = [
        pltpu.make_async_copy(block_of(tok, me, rows), block_of(otok, me, rows), own.at[0]),
        pltpu.make_async_copy(block_of(cot, me, rows), block_of(ocot, me, rows), own.at[1]),
        pltpu.make_async_copy(length, block_of(olen, me, lrows), own.at[2]),
        pltpu.make_async_copy(vec, block_of(ovec, f, vrows), own.at[3]),
    ]
    into = [pltpu.make_async_copy(shard[w], stage[w], own.at[4 + w]) for w in range(weights)]
    for c in local + into:
        c.start()
    out = []
    for w in range(weights):
        into[w].wait()
        c = pltpu.make_async_copy(stage[w], block_of(full[w], f, shard[w].shape[0]), own.at[4 + w])
        c.start()
        out.append(c)

    def step_two(w):
        for d in range(1, F):
            for step in (1, -1):
                row = f - d * step

                @pl.when((row >= 0) & (row < F))
                def _():
                    along(w, row, step).wait_recv()

                    @pl.when((f + step >= 0) & (f + step < F))
                    def _():
                        along(w, row, step).start()

                    across(w, row, 0, False).start()
                    across(w, row, 1, False).start()

    def step_turn(w):
        for j in range(1, F):
            row = lax.rem(f + j, F)
            across(w, row, 0, True).wait_recv()
            across(w, row, 1, True).wait_recv()
            relay(w, row, False).start()

    def step_three(w):
        for j in range(1, F):
            relay(w, lax.rem(f + j, F), True).wait_recv()
            beside(w, j, False).start()

    def step_four(w):
        for j in range(1, F):
            beside(w, j, True).wait_recv()

    steps = (step_two, step_turn, step_three, step_four)
    for at in range(weights + len(steps) - 1):
        for k, step in enumerate(steps):
            if 0 <= at - k < weights:
                step(at - k)
    for w in range(weights):
        for step in (1, -1):

            @pl.when((f + step >= 0) & (f + step < F))
            def _():
                first_along(w, step).wait_send()
                for d in range(1, F):
                    row = f - d * step

                    @pl.when((row >= 0) & (row < F))
                    def _():
                        along(w, row, step).wait_send()

        for j in range(1, F):
            row = lax.rem(f + j, F)
            across(w, row, 0, False).wait_send()
            across(w, row, 1, False).wait_send()
            relay(w, row, False).wait_send()
            beside(w, j, False).wait_send()
    for j in range(1, F):
        vector(j, True).wait()
    for c in local + out:
        c.wait()
    trade_len.wait()
    trade_tok.wait()
    trade_cot.wait()


def fetch(rep_size, fsdp_size, tok, cot, length, vec, shards_in):
    weights = len(shards_in)
    count = rep_size * fsdp_size
    F = fsdp_size
    like = jax.ShapeDtypeStruct
    outs = [
        like(tok.shape, tok.dtype), like(cot.shape, cot.dtype),
        like((count * length.shape[0], length.shape[1]), length.dtype),
        like((F * vec.shape[0], vec.shape[1]), vec.dtype),
    ] + [like((w.shape[0] * F, w.shape[1]), w.dtype) for w in shards_in]
    anywhere = pl.BlockSpec(memory_space=pl.ANY)
    return pl.pallas_call(
        functools.partial(fetch_kernel, rep_size, fsdp_size, weights),
        out_shape=outs,
        in_specs=[anywhere] * (4 + weights),
        out_specs=[anywhere] * (4 + weights),
        scratch_shapes=[pltpu.VMEM(w.shape, w.dtype) for w in shards_in]
        + [DMA((count,))] * 6
        + [DMA((F,))] * 2
        + [DMA((weights, F, 2)), DMA((weights, F))]
        + [DMA((weights, F, 3))] * 2
        + [DMA((weights, F))] * 2
        + [DMA((4 + weights,))],
        compiler_params=pltpu.CompilerParams(collective_id=1, has_side_effects=True),
        name="fetch",
    )(tok, cot, length, vec, *shards_in)


def add_into(dst, left, parts, rows):
    def go(i, carry):
        at = pl.ds(pl.multiple_of(i * rows, rows), rows)
        total = left[at, :].astype(jnp.float32)
        for part in parts:
            total = total + part[at, :].astype(jnp.float32)
        dst[at, :] = total.astype(dst.dtype)
        return carry

    lax.fori_loop(0, dst.shape[0] // rows, go, 0)


def reduce_kernel(rep_size, fsdp_size, weights, *refs):
    F = fsdp_size
    refs = list(refs)
    take = lambda k: [refs.pop(0) for _ in range(k)]
    res, gin = take(2)
    grads = take(weights)
    ores, ogin = take(2)
    owned = take(weights)
    half_in = take(weights)
    half_own = take(weights)
    quad_in = take(weights)
    quad_sum = take(weights)
    line_in = take(weights)
    line_sum = take(weights)
    group_count = rep_size // (2 * QUAD)
    group_in = take(weights) if group_count > 1 else None
    xs, xr, ys, yr, ps, pr, qs, qr, zs, zr, gs, gr, hs, hr, bs, br, own = take(17)
    r, f, core, chip, q, base = position(F)
    count = rep_size * F
    me = r * F + f
    rows = res.shape[0] // count
    enter(count, F, me)

    trade_res = Exchange(count, F, me, res, ores, rows, (xs, xr))
    trade_gin = Exchange(count, F, me, gin, ogin, rows, (ys, yr))
    partner = {"rep": chip * 2 + (1 - core), "fsdp": f}

    def mate(m):
        return {"rep": (base + lax.rem(q + m, QUAD)) * 2 + core, "fsdp": f}

    def columns(ref, w, which):
        half = grads[w].shape[1] // 2
        return ref.at[:, pl.ds(pl.multiple_of(which * half, half), half)]

    def swap(w):
        return remote(columns(grads[w], w, 1 - core), half_in[w], ps.at[w], pr.at[w], partner)

    def size(w):
        S = grads[w].shape[0] // F
        return S, S // QUAD

    near = (flip(q, 1), flip(q, 2))
    far = flip(near[0], 2)

    def chip_at(quarter):
        return {"rep": (base + quarter) * 2 + core, "fsdp": f}

    def rows_of(w, t, quarter):
        S, sq = size(w)
        return pl.ds(pl.multiple_of(t * S + quarter * sq, sq), sq)

    def across(w, t, k):
        side = (w + t) % 2
        return remote(
            half_in[w].at[rows_of(w, t, (near[side], far)[k])], quad_in[w].at[k, t],
            qs.at[w, t, k], qr.at[w, t, k], chip_at(near[side]),
        )

    def turn(w, t):
        side = 1 - (w + t) % 2
        return remote(
            half_in[w].at[rows_of(w, t, near[side])], quad_in[w].at[2, t],
            qs.at[w, t, 2], qr.at[w, t, 2], chip_at(near[side]),
        )

    def along(w, j):
        S, sq = size(w)
        to = lax.rem(f + j, F)
        return remote(
            quad_sum[w].at[pl.ds(pl.multiple_of(to * sq, sq), sq)], line_in[w].at[j - 1],
            zs.at[w, j], zr.at[w, j], {"rep": r, "fsdp": to},
        )

    def group(w, g):
        to = lax.rem(lax.div(chip, QUAD) + g, group_count)
        return remote(
            line_sum[w], group_in[w].at[g - 1], gs.at[w, g], gr.at[w, g],
            {"rep": (to * QUAD + q) * 2 + core, "fsdp": f},
        )

    def home(w, quarter, which):
        S, sq = size(w)
        half = grads[w].shape[1] // 2
        return owned[w].at[
            pl.ds(pl.multiple_of(quarter * sq, sq), sq), pl.ds(pl.multiple_of(which * half, half), half)
        ]

    def spread(w, m, arriving):
        S, sq = size(w)
        return remote(
            line_sum[w], home(w, lax.rem(q + QUAD - m, QUAD) if arriving else q, core),
            hs.at[w, m], hr.at[w, m], mate(m),
        )

    def beside(w, arriving):
        part = columns(owned[w], w, (1 - core) if arriving else core)
        return remote(part, part, bs.at[w], br.at[w], partner)

    for w in range(weights):
        swap(w).start()
    local = [
        pltpu.make_async_copy(block_of(res, me, rows), block_of(ores, me, rows), own.at[0]),
        pltpu.make_async_copy(block_of(gin, me, rows), block_of(ogin, me, rows), own.at[1]),
    ]
    kept = [
        pltpu.make_async_copy(columns(grads[w], w, core), half_own[w], own.at[2 + w])
        for w in range(weights)
    ]
    for c in local + kept:
        c.start()

    def step_one(w):
        kept[w].wait()
        swap(w).wait_recv()
        add_into(half_in[w], half_in[w], [half_own[w]], size(w)[1])
        for t in range(F):
            for k in range(2):
                across(w, t, k).start()

    def step_turn(w):
        for t in range(F):
            for k in range(2):
                across(w, t, k).wait_recv()
            at = rows_of(w, t, near[1 - (w + t) % 2])
            total = half_in[w][at, :].astype(jnp.float32) + quad_in[w][1, t].astype(jnp.float32)
            half_in[w][at, :] = total.astype(half_in[w].dtype)
            turn(w, t).start()

    def step_two(w):
        S, sq = size(w)
        for t in range(F):
            turn(w, t).wait_recv()
            total = half_in[w][rows_of(w, t, q), :].astype(jnp.float32)
            total = total + quad_in[w][0, t].astype(jnp.float32) + quad_in[w][2, t].astype(jnp.float32)
            quad_sum[w][pl.ds(t * sq, sq), :] = total.astype(quad_sum[w].dtype)
        for j in range(1, F):
            along(w, j).start()

    def step_three(w):
        S, sq = size(w)
        for j in range(1, F):
            along(w, j).wait_recv()
        total = quad_sum[w][pl.ds(pl.multiple_of(f * sq, sq), sq), :].astype(jnp.float32)
        for j in range(F - 1):
            total = total + line_in[w][j].astype(jnp.float32)
        line_sum[w][...] = total.astype(line_sum[w].dtype)
        for g in range(1, group_count):
            group(w, g).start()
        if group_count == 1:
            finish(w)

    def step_group(w):
        for g in range(1, group_count):
            group(w, g).wait()
        total = line_sum[w][...].astype(jnp.float32)
        for g in range(group_count - 1):
            total = total + group_in[w][g].astype(jnp.float32)
        line_sum[w][...] = total.astype(line_sum[w].dtype)
        finish(w)

    def finish(w):
        for m in range(1, QUAD):
            spread(w, m, False).start()
        c = pltpu.make_async_copy(line_sum[w], home(w, q, core), own.at[2 + w])
        c.start()
        c.wait()

    def step_four(w):
        for m in range(1, QUAD):
            spread(w, m, True).wait_recv()
        beside(w, False).start()

    steps = [step_one, step_turn, step_two, step_three] + ([step_group] if group_count > 1 else []) + [step_four]
    for at in range(weights + len(steps) - 1):
        for k, step in enumerate(steps):
            if 0 <= at - k < weights:
                step(at - k)
        if at == 0:
            trade_res.start()
            trade_gin.start()
    for w in range(weights):
        beside(w, True).wait_recv()
        swap(w).wait_send()
        for t in range(F):
            across(w, t, 0).wait_send()
            across(w, t, 1).wait_send()
            turn(w, t).wait_send()
        for m in range(1, QUAD):
            spread(w, m, False).wait_send()
        for j in range(1, F):
            along(w, j).wait_send()
        beside(w, False).wait_send()
    for c in local:
        c.wait()
    trade_res.wait()
    trade_gin.wait()


def reduce_all(rep_size, fsdp_size, res, gin, grads):
    weights = len(grads)
    count = rep_size * fsdp_size
    F = fsdp_size
    groups = rep_size // (2 * QUAD)
    like = jax.ShapeDtypeStruct
    anywhere = pl.BlockSpec(memory_space=pl.ANY)
    outs = [like(res.shape, res.dtype), like(gin.shape, gin.dtype)] + [
        like((g.shape[0] // F, g.shape[1]), g.dtype) for g in grads
    ]
    V = pltpu.VMEM
    scratch = [V((g.shape[0], g.shape[1] // 2), g.dtype) for g in grads]
    scratch += [V((g.shape[0], g.shape[1] // 2), g.dtype) for g in grads]
    scratch += [V((3, F, g.shape[0] // QUAD // F, g.shape[1] // 2), g.dtype) for g in grads]
    scratch += [V((g.shape[0] // QUAD, g.shape[1] // 2), g.dtype) for g in grads]
    scratch += [V((F - 1, g.shape[0] // QUAD // F, g.shape[1] // 2), g.dtype) for g in grads]
    scratch += [V((g.shape[0] // QUAD // F, g.shape[1] // 2), g.dtype) for g in grads]
    if groups > 1:
        scratch += [V((groups - 1, g.shape[0] // QUAD // F, g.shape[1] // 2), g.dtype) for g in grads]
    scratch += [DMA((count,))] * 4 + [DMA((weights,))] * 2 + [DMA((weights, F, 3))] * 2
    scratch += [DMA((weights, F))] * 2 + [DMA((weights, max(groups, 2)))] * 2
    scratch += [DMA((weights, QUAD))] * 2 + [DMA((weights,))] * 2 + [DMA((2 + weights,))]
    return pl.pallas_call(
        functools.partial(reduce_kernel, rep_size, fsdp_size, weights),
        out_shape=outs,
        in_specs=[anywhere] * (2 + weights),
        out_specs=[anywhere] * (2 + weights),
        scratch_shapes=scratch,
        compiler_params=pltpu.CompilerParams(
            collective_id=2, has_side_effects=True, vmem_limit_bytes=56 * 2**20
        ),
        name="reduce_all",
    )(res, gin, *grads)


def widen_kernel(count, *refs):
    for k in range(count):
        refs[count + k][...] = refs[k][...].astype(jnp.float32)


def widen(arrays):
    steps = 4

    def spec(a):
        return pl.BlockSpec((a.shape[0] // steps, a.shape[1]), lambda i: (i, 0))

    return pl.pallas_call(
        functools.partial(widen_kernel, len(arrays)),
        grid=(steps,),
        in_specs=[spec(a) for a in arrays],
        out_specs=[spec(a) for a in arrays],
        out_shape=[jax.ShapeDtypeStruct(a.shape, jnp.float32) for a in arrays],
        name="widen",
    )(*arrays)


def matmul(left, right):
    return jnp.dot(left, right, preferred_element_type=jnp.float32)


def matmul_left_t(left, right):
    return lax.dot_general(
        left, right, (((0,), (0,)), ((), ())), preferred_element_type=jnp.float32
    )


def matmul_right_t(left, right):
    return lax.dot_general(
        left, right, (((1,), (1,)), ((), ())), preferred_element_type=jnp.float32
    )


def norm_forward(values, norm_gain, norm_shift):
    center = values - jnp.mean(values, axis=-1, keepdims=True)
    spread = jnp.mean(center * center, axis=-1, keepdims=True)
    scaled_inv = lax.rsqrt(spread + norm_eps)
    normed = center * scaled_inv
    return (normed * norm_gain + norm_shift, normed, scaled_inv)


def norm_backward(grad_out, normed, scaled_inv, norm_gain):
    grad_normed = grad_out * norm_gain
    first_mean = jnp.mean(grad_normed, axis=-1, keepdims=True)
    second_mean = jnp.mean(grad_normed * normed, axis=-1, keepdims=True)
    return (grad_normed - first_mean - normed * second_mean) * scaled_inv


def score_block(query_block, key_rows, kept_keys):
    scores = jnp.einsum(
        "qhd,khd->hqk", query_block, key_rows, preferred_element_type=jnp.float32
    ) * HD ** (-0.5)
    return jnp.where(kept_keys[None, None, :], scores, masked_score)


def attention_forward(query_rows, key_rows, value_rows, kept_keys, block_rows):
    seq_len = query_rows.shape[0]

    def one_block(query_block):
        scores = score_block(query_block, key_rows, kept_keys)
        largest = jnp.max(scores, axis=-1, keepdims=True)
        weights = jnp.exp(scores - largest)
        row_total = jnp.sum(weights, axis=-1, keepdims=True)
        chances = (weights / row_total).astype(jnp.bfloat16)
        context = jnp.einsum(
            "hqk,khd->qhd", chances, value_rows, preferred_element_type=jnp.float32
        )
        return (context, largest + jnp.log(row_total))

    blocks = query_rows.reshape(seq_len // block_rows, block_rows, HEADS, HD)
    context, log_total = lax.map(one_block, blocks)
    return (context.reshape(seq_len, HEADS * HD), log_total)


def attention_backward(
    query_rows, key_rows, value_rows, kept_keys, grad_context, log_total, block_rows
):
    seq_len = query_rows.shape[0]
    block_count = seq_len // block_rows
    scale = HD ** (-0.5)

    def one_block(carry, item):
        grad_keys, grad_values = carry
        query_block, grad_block, log_block = item
        scores = score_block(query_block, key_rows, kept_keys)
        chances = jnp.exp(scores - log_block)
        grad_chances = jnp.einsum(
            "qhd,khd->hqk", grad_block, value_rows, preferred_element_type=jnp.float32
        )
        centered = jnp.sum(chances * grad_chances, axis=-1, keepdims=True)
        grad_scores = (chances * (grad_chances - centered)).astype(jnp.bfloat16)
        grad_query = (
            jnp.einsum("hqk,khd->qhd", grad_scores, key_rows, preferred_element_type=jnp.float32)
            * scale
        )
        grad_keys = (
            grad_keys
            + jnp.einsum(
                "hqk,qhd->khd", grad_scores, query_block, preferred_element_type=jnp.float32
            )
            * scale
        )
        grad_values = grad_values + jnp.einsum(
            "hqk,qhd->khd",
            chances.astype(jnp.bfloat16),
            grad_block,
            preferred_element_type=jnp.float32,
        )
        return ((grad_keys, grad_values), grad_query)

    start = jnp.zeros(key_rows.shape, jnp.float32)
    items = (
        query_rows.reshape(block_count, block_rows, HEADS, HD),
        grad_context.reshape(block_count, block_rows, HEADS, HD),
        log_total,
    )
    (grad_keys, grad_values), grad_query = lax.scan(one_block, (start, start), items)
    return (
        grad_query.reshape(seq_len, HEADS * HD),
        grad_keys.reshape(seq_len, HEADS * HD),
        grad_values.reshape(seq_len, HEADS * HD),
    )


def shards(
    tokens,
    cotangent,
    lengths,
    slot_seq,
    query_weight,
    query_bias,
    key_weight,
    value_weight,
    value_bias,
    out_weight,
    out_bias,
    first_gain,
    first_shift,
    inner_weight,
    inner_bias,
    outer_weight,
    outer_bias,
    second_gain,
    second_shift,
):
    rep_size, fsdp_size = lax.axis_size("rep"), lax.axis_size("fsdp")
    me = lax.axis_index("rep") * fsdp_size + lax.axis_index("fsdp")
    row_count, feature_dim = tokens.shape
    small = [query_bias, value_bias, out_bias, first_gain, first_shift, outer_bias, second_gain, second_shift]
    width = query_bias.shape[0]
    wide = inner_bias.shape[0] // width
    lanes = 256
    vec_rows = 16

    def stack(vectors):
        table = jnp.stack([v.reshape(width) for v in vectors])
        return jnp.pad(table, ((0, vec_rows - table.shape[0]), (0, lanes - width)))

    vec = stack(small + list(inner_bias.reshape(wide, width)))
    length_block = jnp.broadcast_to(lengths.reshape(1, 1), (8, 128))
    (
        seq_rows, seq_seed, all_lengths, all_vec,
        query_full, key_full, value_full, out_full, inner_full, outer_full,
    ) = fetch(
        rep_size, fsdp_size, tokens, cotangent, length_block, vec,
        [query_weight, key_weight, value_weight, out_weight, inner_weight, outer_weight],
    )
    my_length = all_lengths.reshape(-1, 8, 128)[slot_seq[me], 0, 0]
    kept = jnp.arange(row_count, dtype=jnp.int32) < my_length
    table = all_vec.reshape(fsdp_size, vec_rows, lanes)[:, :, :width].astype(jnp.float32)
    (
        query_bias_full, value_bias_full, out_bias_full, first_gain_full, first_shift_full,
        outer_bias_full, second_gain_full, second_shift_full,
    ) = [table[:, i].reshape(-1) for i in range(8)]
    inner_bias_full = table[:, 8 : 8 + wide].reshape(-1)
    block_rows = math.gcd(row_count, 512)
    head_shape = (row_count, HEADS, HD)
    query_rows = (
        (matmul(seq_rows, query_full) + query_bias_full).astype(jnp.bfloat16).reshape(head_shape)
    )
    key_rows = matmul(seq_rows, key_full).astype(jnp.bfloat16).reshape(head_shape)
    value_rows = (
        (matmul(seq_rows, value_full) + value_bias_full).astype(jnp.bfloat16).reshape(head_shape)
    )
    context, log_total = attention_forward(query_rows, key_rows, value_rows, kept, block_rows)
    context = context.astype(jnp.bfloat16)
    attended = matmul(context, out_full) + out_bias_full
    hidden, first_normed, first_inv = norm_forward(
        seq_rows.astype(jnp.float32) + attended, first_gain_full, first_shift_full
    )
    hidden_low = hidden.astype(jnp.bfloat16)
    inner = matmul(hidden_low, inner_full) + inner_bias_full
    activated = jax.nn.gelu(inner, approximate=False).astype(jnp.bfloat16)
    outer = matmul(activated, outer_full) + outer_bias_full
    result, second_normed, second_inv = norm_forward(
        hidden + outer, second_gain_full, second_shift_full
    )
    result = jnp.where(kept[:, None], result, 0.0).astype(jnp.bfloat16)
    seed_rows = jnp.where(kept[:, None], seq_seed.astype(jnp.float32), 0.0)
    grad_second_gain = jnp.sum(seed_rows * second_normed, axis=0)
    grad_second_shift = jnp.sum(seed_rows, axis=0)
    grad_second = norm_backward(seed_rows, second_normed, second_inv, second_gain_full)
    grad_outer = grad_second.astype(jnp.bfloat16)
    grad_outer_bias = jnp.sum(grad_outer, axis=0, dtype=jnp.float32)
    grad_outer_weight = matmul_left_t(activated, grad_outer)
    grad_activated = matmul_right_t(grad_outer, outer_full)
    slope = (
        0.5 * (1.0 + lax.erf(inner * inv_root_two))
        + inner * jnp.exp(-0.5 * inner * inner) * inv_root_two_pi
    )
    grad_inner = (grad_activated * slope).astype(jnp.bfloat16)
    grad_inner_bias = jnp.sum(grad_inner, axis=0, dtype=jnp.float32)
    grad_inner_weight = matmul_left_t(hidden_low, grad_inner)
    grad_hidden = grad_second + matmul_right_t(grad_inner, inner_full)
    grad_first_gain = jnp.sum(grad_hidden * first_normed, axis=0)
    grad_first_shift = jnp.sum(grad_hidden, axis=0)
    grad_residual = norm_backward(grad_hidden, first_normed, first_inv, first_gain_full)
    grad_attended = grad_residual.astype(jnp.bfloat16)
    grad_out_bias = jnp.sum(grad_attended, axis=0, dtype=jnp.float32)
    grad_out_weight = matmul_left_t(context, grad_attended)
    grad_context = matmul_right_t(grad_attended, out_full).astype(jnp.bfloat16)
    grad_query, grad_key, grad_value = attention_backward(
        query_rows, key_rows, value_rows, kept, grad_context.reshape(head_shape), log_total, block_rows
    )
    grad_query = grad_query.astype(jnp.bfloat16)
    grad_key = grad_key.astype(jnp.bfloat16)
    grad_value = grad_value.astype(jnp.bfloat16)
    grad_query_bias = jnp.sum(grad_query, axis=0, dtype=jnp.float32)
    grad_value_bias = jnp.sum(grad_value, axis=0, dtype=jnp.float32)
    grad_query_weight = matmul_left_t(seq_rows, grad_query)
    grad_key_weight = matmul_left_t(seq_rows, grad_key)
    grad_value_weight = matmul_left_t(seq_rows, grad_value)
    grad_input = (
        grad_residual
        + matmul_right_t(grad_query, query_full)
        + matmul_right_t(grad_key, key_full)
        + matmul_right_t(grad_value, value_full)
    ).astype(jnp.bfloat16)
    low = lambda g: g.astype(jnp.bfloat16)
    grad_small = [
        grad_query_bias, grad_value_bias, grad_out_bias, grad_first_gain, grad_first_shift,
        grad_outer_bias, grad_second_gain, grad_second_shift,
    ]
    grad_table = jnp.concatenate(
        [
            jnp.stack(grad_small).reshape(8, fsdp_size, width).transpose(1, 0, 2),
            grad_inner_bias.reshape(fsdp_size, wide, width),
        ],
        axis=1,
    )
    grad_rows = 32
    grad_table = jnp.pad(
        grad_table, ((0, 0), (0, grad_rows - 8 - wide), (0, lanes - width))
    ).reshape(fsdp_size * grad_rows, lanes)
    (
        back_rows, back_grads, d_outer, d_inner, d_out, d_query, d_key, d_value, d_vec,
    ) = reduce_all(
        rep_size, fsdp_size, result, grad_input,
        [
            low(grad_outer_weight), low(grad_inner_weight), low(grad_out_weight),
            low(grad_query_weight), low(grad_key_weight), low(grad_value_weight), grad_table,
        ],
    )
    d_outer, d_inner, d_out, d_query, d_key, d_value = widen(
        [d_outer, d_inner, d_out, d_query, d_key, d_value]
    )
    v = d_vec[:, :width]
    return (
        back_rows, back_grads,
        d_query, v[0], d_key, d_value, v[1], d_out, v[2], v[3], v[4],
        d_inner, v[8 : 8 + wide].reshape(-1), d_outer, v[5], v[6], v[7],
    )


def solution(mesh):
    placed = (
        P(("rep", "fsdp"), None),
        P(("rep", "fsdp"), None),
        P(("rep", "fsdp")),
        P(),
        P("fsdp", None),
        P("fsdp"),
        P("fsdp", None),
        P("fsdp", None),
        P("fsdp"),
        P("fsdp", None),
        P("fsdp"),
        P("fsdp"),
        P("fsdp"),
        P("fsdp", None),
        P("fsdp"),
        P("fsdp", None),
        P("fsdp"),
        P("fsdp"),
        P("fsdp"),
    )
    return jax.shard_map(
        shards,
        mesh=mesh,
        in_specs=placed,
        out_specs=(
            P(("rep", "fsdp"), None),
            P(("rep", "fsdp"), None),
            P("fsdp", None),
            P("fsdp"),
            P("fsdp", None),
            P("fsdp", None),
            P("fsdp"),
            P("fsdp", None),
            P("fsdp"),
            P("fsdp"),
            P("fsdp"),
            P("fsdp", None),
            P("fsdp"),
            P("fsdp", None),
            P("fsdp"),
            P("fsdp"),
            P("fsdp"),
        ),
        check_vma=False,
    )
```

```python
import functools

import jax
import jax.numpy as jnp
from jax import lax
from jax.experimental import pallas as pl
from jax.experimental.pallas import tpu as pltpu
from jax.sharding import PartitionSpec as P

HEADS = 12
HD = 64
MESH = pl.DeviceIdType.MESH
DMA = pltpu.SemaphoreType.DMA
QUAD = 4
SAVED = 14


norm_eps = 1e-12
masked_score = -1e30
inv_root_two = 0.7071067811865476
inv_root_two_pi = 0.3989422804014327


def remote(src, dst, send, recv, device):
    return pltpu.make_async_remote_copy(
        src_ref=src, dst_ref=dst, send_sem=send, recv_sem=recv,
        device_id=device, device_id_type=MESH,
    )


def place(linear, fsdp_size):
    return {"rep": lax.div(linear, fsdp_size), "fsdp": lax.rem(linear, fsdp_size)}


def enter(count, fsdp_size, me):
    sem = pltpu.get_barrier_semaphore()

    def greet(k, carry):
        pl.semaphore_signal(
            sem, inc=1, device_id=place(lax.rem(me + k, count), fsdp_size), device_id_type=MESH
        )
        return carry

    lax.fori_loop(1, count, greet, 0)
    pl.semaphore_wait(sem, count - 1)


class Exchange:
    def __init__(self, count, fsdp_size, me, src, dst, rows, sems, spread=False):
        self.args = (count, fsdp_size, me, src, dst, rows, sems, spread)

    def copy(self, k, arriving):
        count, fsdp_size, me, src, dst, rows, (send, recv), spread = self.args
        peer = lax.rem(me + k, count)
        slot = lax.rem(me + count - k, count) if arriving else me
        source = src if spread else src.at[pl.ds(pl.multiple_of(peer * rows, rows), rows)]
        return remote(
            source, dst.at[pl.ds(pl.multiple_of(slot * rows, rows), rows)],
            send.at[k], recv.at[k], place(peer, fsdp_size),
        )

    def start(self):
        def go(k, carry):
            self.copy(k, False).start()
            return carry

        lax.fori_loop(1, self.args[0], go, 0)

    def wait(self):
        def go(k, carry):
            self.copy(k, True).wait()
            return carry

        lax.fori_loop(1, self.args[0], go, 0)


def block_of(ref, index, rows):
    return ref.at[pl.ds(pl.multiple_of(index * rows, rows), rows)]


def position(fsdp_size):
    r = lax.axis_index("rep")
    f = lax.axis_index("fsdp")
    core = lax.rem(r, 2)
    chip = lax.div(r, 2)
    q = lax.rem(chip, QUAD)
    return r, f, core, chip, q, chip - q


def flip(q, bit):
    return q + bit - 2 * bit * lax.rem(lax.div(q, bit), 2)


def fetch_kernel(rep_size, fsdp_size, weights, *refs):
    F = fsdp_size
    refs = list(refs)
    take = lambda k: [refs.pop(0) for _ in range(k)]
    slots, tok, cot, length, vec = take(5)
    shard = take(weights)
    otok, ocot, ovec = take(3)
    full = take(weights)
    saved = take(SAVED)
    olen = take(1)[0]
    stage = take(weights)
    held = take(weights)
    x_v, len_v, vec_v, par_v = take(4)
    keep = take(SAVED)
    load_sem, save_sem = take(2)
    (query_v, key_v, value_v, prob_v, context_v, norm1_v, inv1_v, low_v, act_v, slope_v, norm2_v,
     inv2_v, result_v, keptv) = keep
    xs, xr, ys, yr, ls, lr, vs, vr, zs, zr, qs, qr, ps, pr, own = take(15)
    r, f, core, chip, q, base = position(F)
    count = rep_size * F
    me = r * F + f
    rows = tok.shape[0] // count
    vrows = vec.shape[0]
    lrows = length.shape[0]
    enter(count, F, me)

    trade_tok = Exchange(count, F, me, tok, otok, rows, (xs, xr))
    trade_cot = Exchange(count, F, me, cot, ocot, rows, (ys, yr))
    trade_len = Exchange(count, F, me, length, olen, lrows, (ls, lr), spread=True)

    def piece(ref, w, shard_row, quarter):
        S, C = shard[w].shape
        sq, half = S // QUAD, C // 2
        return ref.at[
            pl.ds(pl.multiple_of(shard_row * S + quarter * sq, sq), sq),
            pl.ds(pl.multiple_of(core * half, half), half),
        ]

    def strip(w, shard_row, which):
        S, C = shard[w].shape
        half = C // 2
        return full[w].at[
            pl.ds(pl.multiple_of(shard_row * S, S), S), pl.ds(pl.multiple_of(which * half, half), half)
        ]

    near = (flip(q, 1), flip(q, 2))
    far = flip(near[0], 2)

    def chip_at(quarter):
        return {"rep": (base + quarter) * 2 + core, "fsdp": f}

    partner = {"rep": chip * 2 + (1 - core), "fsdp": f}

    def along(w, row, step):
        source = piece(full[w], w, row, q)
        return remote(
            source, source, zs.at[w, row, (1 - step) // 2], zr.at[w, row], {"rep": r, "fsdp": f + step}
        )

    def first_along(w, step):
        return remote(
            piece(shard[w], w, 0, q), piece(full[w], w, f, q),
            zs.at[w, f, (1 - step) // 2], zr.at[w, f], {"rep": r, "fsdp": f + step},
        )

    def across(w, row, side, arriving):
        part = piece(full[w], w, row, near[side] if arriving else q)
        return remote(part, part, qs.at[w, row, side], qr.at[w, row, side], chip_at(near[side]))

    def relay(w, row, arriving):
        turn = lax.rem(row + w, 2)
        part = piece(full[w], w, row, far if arriving else jnp.where(turn == 0, near[1], near[0]))
        to = chip_at(jnp.where(turn == 0, near[0], near[1]))
        return remote(part, part, qs.at[w, row, 2], qr.at[w, row, 2], to)

    def beside(w, j, arriving):
        row = lax.rem(f + j, F)
        part = strip(w, row, (1 - core) if arriving else core)
        return remote(part, part, ps.at[w, j], pr.at[w, j], partner)

    def vector(j, arriving):
        to = lax.rem(f + j, F)
        row = lax.rem(f + F - j, F) if arriving else f
        return remote(vec, block_of(ovec, row, vrows), vs.at[j], vr.at[j], {"rep": r, "fsdp": to})

    trade_len.start()
    for j in range(1, F):
        vector(j, False).start()
    trade_tok.start()
    for w in range(weights):
        @pl.when(f < F - 1)
        def _():
            first_along(w, 1).start()

        @pl.when(f > 0)
        def _():
            first_along(w, -1).start()

    local = [
        pltpu.make_async_copy(block_of(tok, me, rows), block_of(otok, me, rows), own.at[0]),
        pltpu.make_async_copy(block_of(cot, me, rows), block_of(ocot, me, rows), own.at[1]),
        pltpu.make_async_copy(length, block_of(olen, me, lrows), own.at[2]),
        pltpu.make_async_copy(vec, block_of(ovec, f, vrows), own.at[3]),
    ]
    into = [pltpu.make_async_copy(shard[w], stage[w], own.at[4 + w]) for w in range(weights)]
    for c in local + into:
        c.start()
    out = []
    for w in range(weights):
        into[w].wait()
        c = pltpu.make_async_copy(stage[w], block_of(full[w], f, shard[w].shape[0]), own.at[4 + w])
        c.start()
        out.append(c)

    def step_two(w):
        for d in range(1, F):
            for step in (1, -1):
                row = f - d * step

                @pl.when((row >= 0) & (row < F))
                def _():
                    along(w, row, step).wait_recv()

                    @pl.when((f + step >= 0) & (f + step < F))
                    def _():
                        along(w, row, step).start()

                    across(w, row, 0, False).start()
                    across(w, row, 1, False).start()

    def step_turn(w):
        for j in range(1, F):
            row = lax.rem(f + j, F)
            across(w, row, 0, True).wait_recv()
            across(w, row, 1, True).wait_recv()
            relay(w, row, False).start()

    def step_three(w):
        for j in range(1, F):
            relay(w, lax.rem(f + j, F), True).wait_recv()
            beside(w, j, False).start()

    def step_four(w):
        for j in range(1, F):
            beside(w, j, True).wait_recv()

    steps = (step_two, step_turn, step_three, step_four)

    def advance(at):
        for k, step in enumerate(steps):
            if 0 <= at - k < weights:
                step(at - k)
        done = at - len(steps) + 1
        if 0 <= done < weights:
            out[done].wait()
            pltpu.make_async_copy(full[done], held[done], load_sem.at[done]).start()

    def ready(w):
        pltpu.make_async_copy(full[w], held[w], load_sem.at[w]).wait()

    def store(k):
        pltpu.make_async_copy(keep[k], saved[k], save_sem.at[k]).start()

    n_rows, width = x_v.shape
    f32, bf16 = jnp.float32, jnp.bfloat16

    def project(dst, w, bias):
        tile = 256

        def go(i, carry):
            at = pl.ds(pl.multiple_of(i * tile, tile), tile)
            total = jnp.dot(x_v[...], held[w][:, at], preferred_element_type=f32)
            if bias is not None:
                total = total + par_v[bias : bias + 1, at]
            dst[:, at] = total.astype(bf16)
            return carry

        lax.fori_loop(0, width // tile, go, 0)

    def attend(first, last):
        block = 256
        blocks = n_rows // block

        def go(i, carry):
            pair = lax.div(i, blocks)
            rows_at = pl.ds(pl.multiple_of(lax.rem(i, blocks) * block, block), block)
            lanes = pl.ds(pl.multiple_of(pair * 128, 128), 128)
            lane = lax.broadcasted_iota(jnp.int32, (n_rows, 128), 1)
            queries = query_v[rows_at, lanes]
            keys = key_v[:, lanes]
            values = value_v[:, lanes]
            seen = keptv[0:1, :]
            total = jnp.zeros((block, 128), f32)
            for side in range(2):
                mine = (lane >= side * HD) & (lane < side * HD + HD)
                k_side = jnp.where(mine, keys, jnp.zeros_like(keys))
                v_side = jnp.where(mine, values, jnp.zeros_like(values))
                scores = matmul_right_t(queries, k_side) * HD ** (-0.5)
                scores = jnp.where(seen > 0, scores, masked_score)
                largest = jnp.max(scores, axis=-1, keepdims=True)
                powers = jnp.exp(scores - largest)
                probs = (powers * (1.0 / jnp.sum(powers, axis=-1, keepdims=True))).astype(bf16)
                prob_v[pair * 2 + side, rows_at, :] = probs
                total = total + jnp.dot(probs, v_side, preferred_element_type=f32)
            context_v[rows_at, lanes] = total.astype(bf16)
            return carry

        lax.fori_loop(first * blocks, last * blocks, go, 0)

    def normalize(values):
        center = values - jnp.mean(values, axis=-1, keepdims=True)
        inv = lax.rsqrt(jnp.mean(center * center, axis=-1, keepdims=True) + norm_eps)
        return center * inv, inv

    def first_half():
        block = 128

        def go(i, carry):
            at = pl.ds(pl.multiple_of(i * block, block), block)
            total = jnp.dot(context_v[at, :], held[3][...], preferred_element_type=f32)
            normed, inv = normalize(x_v[at, :].astype(f32) + (total + par_v[2:3, :width]))
            norm1_v[at, :] = normed
            inv1_v[at, :] = jnp.broadcast_to(inv, (block, 128))
            low_v[at, :] = (normed * par_v[3:4, :width] + par_v[4:5, :width]).astype(bf16)
            return carry

        lax.fori_loop(0, n_rows // block, go, 0)

    def widen_out(first, last):
        tile = 256

        def go(i, carry):
            at = pl.ds(pl.multiple_of(i * tile, tile), tile)
            block = 256

            def rows_go(k, c2):
                rows_at = pl.ds(pl.multiple_of(k * block, block), block)
                inner = jnp.dot(low_v[rows_at, :], held[4][:, at], preferred_element_type=f32)
                inner = inner + par_v[8:9, at]
                share = 0.5 * (1.0 + lax.erf(inner * inv_root_two))
                act_v[rows_at, at] = (inner * share).astype(bf16)
                slope = share + inner * jnp.exp(-0.5 * inner * inner) * inv_root_two_pi
                slope_v[rows_at, at] = slope.astype(bf16)
                return c2

            lax.fori_loop(0, n_rows // block, rows_go, 0)
            return carry

        lax.fori_loop(first, last, go, 0)

    def second_half():
        block = 128

        def go(i, carry):
            at = pl.ds(pl.multiple_of(i * block, block), block)
            total = jnp.dot(act_v[at, :], held[5][...], preferred_element_type=f32)
            hidden = norm1_v[at, :] * par_v[3:4, :width] + par_v[4:5, :width]
            normed, inv = normalize(hidden + (total + par_v[5:6, :width]))
            norm2_v[at, :] = normed
            inv2_v[at, :] = jnp.broadcast_to(inv, (block, 128))
            row = lax.broadcasted_iota(jnp.int32, (block, 1), 0) + i * block
            live = row < jnp.max(keptv[1:2, 0:1])
            result = normed * par_v[6:7, :width] + par_v[7:8, :width]
            result_v[at, :] = jnp.where(live, result, 0.0).astype(bf16)
            return carry

        lax.fori_loop(0, n_rows // block, go, 0)
        for k in (10, 11, 12):
            store(k)

    advance(0)
    advance(1)
    advance(2)
    for j in range(1, F):
        vector(j, True).wait()
    trade_len.wait()
    trade_tok.wait()
    for c in local:
        c.wait()
    fill = [
        pltpu.make_async_copy(otok, x_v, load_sem.at[weights]),
        pltpu.make_async_copy(olen, len_v, load_sem.at[weights + 1]),
        pltpu.make_async_copy(ovec, vec_v, load_sem.at[weights + 2]),
    ]
    for c in fill:
        c.start()
    for c in fill:
        c.wait()
    narrow = jnp.zeros((8, width), f32)
    for k in range(F):
        narrow = narrow + vec_v[k * vrows : k * vrows + 16, :].astype(f32)[0:8, :]
    par_v[0:8, 0:width] = narrow
    part = shard[5].shape[0]
    for k in range(F):
        par_v[8:9, k * part : (k + 1) * part] = vec_v[k * vrows : k * vrows + 16, :].astype(f32)[8:9, 0:part]
    mine = slots[me]
    owner = lax.div(lax.broadcasted_iota(jnp.int32, len_v.shape, 0), lrows)
    my_length = jnp.max(jnp.where(owner == mine, len_v[...], 0))
    key_at = lax.broadcasted_iota(jnp.int32, (8, n_rows), 1)
    second = lax.broadcasted_iota(jnp.int32, (8, n_rows), 0) > 0
    keptv[...] = jnp.where(second, my_length, (key_at < my_length).astype(jnp.int32))
    advance(3)
    ready(0)
    project(query_v, 0, 0)
    advance(4)
    ready(1)
    project(key_v, 1, None)
    advance(5)
    trade_cot.start()
    ready(2)
    project(value_v, 2, 1)
    for k in (0, 1, 2):
        store(k)
    attend(0, 2)
    advance(6)
    attend(2, 4)
    advance(7)
    attend(4, 6)
    for k in (3, 4):
        store(k)
    ready(3)
    first_half()
    for k in (5, 6, 7):
        store(k)
    tiles = held[4].shape[1] // 256
    ready(4)
    widen_out(0, tiles // 2)
    advance(8)
    widen_out(tiles // 2, tiles)
    for k in (8, 9):
        store(k)
    ready(5)
    second_half()
    store(13)
    for w in range(weights):
        for step in (1, -1):

            @pl.when((f + step >= 0) & (f + step < F))
            def _():
                first_along(w, step).wait_send()
                for d in range(1, F):
                    row = f - d * step

                    @pl.when((row >= 0) & (row < F))
                    def _():
                        along(w, row, step).wait_send()

        for j in range(1, F):
            row = lax.rem(f + j, F)
            across(w, row, 0, False).wait_send()
            across(w, row, 1, False).wait_send()
            relay(w, row, False).wait_send()
            beside(w, j, False).wait_send()
    trade_cot.wait()
    for k in range(SAVED):
        pltpu.make_async_copy(keep[k], saved[k], save_sem.at[k]).wait()


def fetch(rep_size, fsdp_size, slots, tok, cot, length, vec, shards_in):
    weights = len(shards_in)
    count = rep_size * fsdp_size
    F = fsdp_size
    like = jax.ShapeDtypeStruct
    n_rows, width = tok.shape
    hidden_width = shards_in[4].shape[1]
    bf16, f32 = jnp.bfloat16, jnp.float32
    rows_of = lambda columns, kind: like((n_rows, columns), kind)
    save = [rows_of(width, bf16)] * 3 + [like((HEADS, n_rows, n_rows), bf16), rows_of(width, bf16)]
    save += [rows_of(width, f32), rows_of(128, f32), rows_of(width, bf16)]
    save += [rows_of(hidden_width, bf16)] * 2 + [rows_of(width, f32), rows_of(128, f32), rows_of(width, bf16)]
    save += [like((8, n_rows), jnp.int32)]
    wide = [like((w.shape[0] * F, w.shape[1]), w.dtype) for w in shards_in]
    outs = [
        like(tok.shape, tok.dtype), like(cot.shape, cot.dtype),
        like((F * vec.shape[0], vec.shape[1]), vec.dtype),
    ] + wide + save + [like((count * length.shape[0], length.shape[1]), length.dtype)]
    anywhere = pl.BlockSpec(memory_space=pl.ANY)
    V = lambda a: pltpu.VMEM(a.shape, a.dtype)
    return pl.pallas_call(
        functools.partial(fetch_kernel, rep_size, fsdp_size, weights),
        out_shape=outs,
        in_specs=[pl.BlockSpec(memory_space=pltpu.SMEM)] + [anywhere] * (4 + weights),
        out_specs=[anywhere] * len(outs),
        scratch_shapes=[V(w) for w in shards_in]
        + [V(w) for w in wide]
        + [V(tok), V(outs[-1]), V(outs[2]), pltpu.VMEM((16, hidden_width), f32)]
        + [V(a) for a in save]
        + [DMA((weights + 3,)), DMA((SAVED,))]
        + [DMA((count,))] * 6
        + [DMA((F,))] * 2
        + [DMA((weights, F, 2)), DMA((weights, F))]
        + [DMA((weights, F, 3))] * 2
        + [DMA((weights, F))] * 2
        + [DMA((4 + weights,))],
        compiler_params=pltpu.CompilerParams(
            collective_id=1, has_side_effects=True, vmem_limit_bytes=60 * 2**20
        ),
        name="forward",
    )(slots, tok, cot, length, vec, *shards_in)


def add_into(dst, left, parts, rows):
    def go(i, carry):
        at = pl.ds(pl.multiple_of(i * rows, rows), rows)
        total = left[at, :].astype(jnp.float32)
        for part in parts:
            total = total + part[at, :].astype(jnp.float32)
        dst[at, :] = total.astype(dst.dtype)
        return carry

    lax.fori_loop(0, dst.shape[0] // rows, go, 0)


def reduce_kernel(rep_size, fsdp_size, weights, *refs):
    F = fsdp_size
    refs = list(refs)
    take = lambda k: [refs.pop(0) for _ in range(k)]
    res, gin = take(2)
    grads = take(weights)
    ores, ogin = take(2)
    owned = take(weights)
    half_in = take(weights)
    half_own = take(weights)
    quad_in = take(weights)
    quad_sum = take(weights)
    line_in = take(weights)
    line_sum = take(weights)
    group_count = rep_size // (2 * QUAD)
    group_in = take(weights) if group_count > 1 else None
    xs, xr, ys, yr, ps, pr, qs, qr, zs, zr, gs, gr, hs, hr, bs, br, own = take(17)
    r, f, core, chip, q, base = position(F)
    count = rep_size * F
    me = r * F + f
    rows = res.shape[0] // count
    enter(count, F, me)

    trade_res = Exchange(count, F, me, res, ores, rows, (xs, xr))
    trade_gin = Exchange(count, F, me, gin, ogin, rows, (ys, yr))
    partner = {"rep": chip * 2 + (1 - core), "fsdp": f}

    def mate(m):
        return {"rep": (base + lax.rem(q + m, QUAD)) * 2 + core, "fsdp": f}

    def columns(ref, w, which):
        half = grads[w].shape[1] // 2
        return ref.at[:, pl.ds(pl.multiple_of(which * half, half), half)]

    def swap(w):
        return remote(columns(grads[w], w, 1 - core), half_in[w], ps.at[w], pr.at[w], partner)

    def size(w):
        S = grads[w].shape[0] // F
        return S, S // QUAD

    near = (flip(q, 1), flip(q, 2))
    far = flip(near[0], 2)

    def chip_at(quarter):
        return {"rep": (base + quarter) * 2 + core, "fsdp": f}

    def rows_of(w, t, quarter):
        S, sq = size(w)
        return pl.ds(pl.multiple_of(t * S + quarter * sq, sq), sq)

    def across(w, t, k):
        side = (w + t) % 2
        return remote(
            half_in[w].at[rows_of(w, t, (near[side], far)[k])], quad_in[w].at[k, t],
            qs.at[w, t, k], qr.at[w, t, k], chip_at(near[side]),
        )

    def turn(w, t):
        side = 1 - (w + t) % 2
        return remote(
            half_in[w].at[rows_of(w, t, near[side])], quad_in[w].at[2, t],
            qs.at[w, t, 2], qr.at[w, t, 2], chip_at(near[side]),
        )

    def along(w, j):
        S, sq = size(w)
        to = lax.rem(f + j, F)
        return remote(
            quad_sum[w].at[pl.ds(pl.multiple_of(to * sq, sq), sq)], line_in[w].at[j - 1],
            zs.at[w, j], zr.at[w, j], {"rep": r, "fsdp": to},
        )

    def group(w, g):
        to = lax.rem(lax.div(chip, QUAD) + g, group_count)
        return remote(
            line_sum[w], group_in[w].at[g - 1], gs.at[w, g], gr.at[w, g],
            {"rep": (to * QUAD + q) * 2 + core, "fsdp": f},
        )

    def home(w, quarter, which):
        S, sq = size(w)
        half = grads[w].shape[1] // 2
        return owned[w].at[
            pl.ds(pl.multiple_of(quarter * sq, sq), sq), pl.ds(pl.multiple_of(which * half, half), half)
        ]

    def spread(w, m, arriving):
        S, sq = size(w)
        return remote(
            line_sum[w], home(w, lax.rem(q + QUAD - m, QUAD) if arriving else q, core),
            hs.at[w, m], hr.at[w, m], mate(m),
        )

    def beside(w, arriving):
        part = columns(owned[w], w, (1 - core) if arriving else core)
        return remote(part, part, bs.at[w], br.at[w], partner)

    for w in range(weights):
        swap(w).start()
    local = [
        pltpu.make_async_copy(block_of(res, me, rows), block_of(ores, me, rows), own.at[0]),
        pltpu.make_async_copy(block_of(gin, me, rows), block_of(ogin, me, rows), own.at[1]),
    ]
    kept = [
        pltpu.make_async_copy(columns(grads[w], w, core), half_own[w], own.at[2 + w])
        for w in range(weights)
    ]
    for c in local + kept:
        c.start()

    def step_one(w):
        kept[w].wait()
        swap(w).wait_recv()
        add_into(half_in[w], half_in[w], [half_own[w]], size(w)[1])
        for t in range(F):
            for k in range(2):
                across(w, t, k).start()

    def step_turn(w):
        for t in range(F):
            for k in range(2):
                across(w, t, k).wait_recv()
            at = rows_of(w, t, near[1 - (w + t) % 2])
            total = half_in[w][at, :].astype(jnp.float32) + quad_in[w][1, t].astype(jnp.float32)
            half_in[w][at, :] = total.astype(half_in[w].dtype)
            turn(w, t).start()

    def step_two(w):
        S, sq = size(w)
        for t in range(F):
            turn(w, t).wait_recv()
            total = half_in[w][rows_of(w, t, q), :].astype(jnp.float32)
            total = total + quad_in[w][0, t].astype(jnp.float32) + quad_in[w][2, t].astype(jnp.float32)
            quad_sum[w][pl.ds(t * sq, sq), :] = total.astype(quad_sum[w].dtype)
        for j in range(1, F):
            along(w, j).start()

    def step_three(w):
        S, sq = size(w)
        for j in range(1, F):
            along(w, j).wait_recv()
        total = quad_sum[w][pl.ds(pl.multiple_of(f * sq, sq), sq), :].astype(jnp.float32)
        for j in range(F - 1):
            total = total + line_in[w][j].astype(jnp.float32)
        line_sum[w][...] = total.astype(line_sum[w].dtype)
        for g in range(1, group_count):
            group(w, g).start()
        if group_count == 1:
            finish(w)

    def step_group(w):
        for g in range(1, group_count):
            group(w, g).wait()
        total = line_sum[w][...].astype(jnp.float32)
        for g in range(group_count - 1):
            total = total + group_in[w][g].astype(jnp.float32)
        line_sum[w][...] = total.astype(line_sum[w].dtype)
        finish(w)

    def finish(w):
        for m in range(1, QUAD):
            spread(w, m, False).start()
        c = pltpu.make_async_copy(line_sum[w], home(w, q, core), own.at[2 + w])
        c.start()
        c.wait()

    def step_four(w):
        for m in range(1, QUAD):
            spread(w, m, True).wait_recv()
        beside(w, False).start()

    steps = [step_one, step_turn, step_two, step_three] + ([step_group] if group_count > 1 else []) + [step_four]
    for at in range(weights + len(steps) - 1):
        for k, step in enumerate(steps):
            if 0 <= at - k < weights:
                step(at - k)
        if at == 0:
            trade_res.start()
            trade_gin.start()
    for w in range(weights):
        beside(w, True).wait_recv()
        swap(w).wait_send()
        for t in range(F):
            across(w, t, 0).wait_send()
            across(w, t, 1).wait_send()
            turn(w, t).wait_send()
        for m in range(1, QUAD):
            spread(w, m, False).wait_send()
        for j in range(1, F):
            along(w, j).wait_send()
        beside(w, False).wait_send()
    for c in local:
        c.wait()
    trade_res.wait()
    trade_gin.wait()


def reduce_all(rep_size, fsdp_size, res, gin, grads):
    weights = len(grads)
    count = rep_size * fsdp_size
    F = fsdp_size
    groups = rep_size // (2 * QUAD)
    like = jax.ShapeDtypeStruct
    anywhere = pl.BlockSpec(memory_space=pl.ANY)
    outs = [like(res.shape, res.dtype), like(gin.shape, gin.dtype)] + [
        like((g.shape[0] // F, g.shape[1]), g.dtype) for g in grads
    ]
    V = pltpu.VMEM
    scratch = [V((g.shape[0], g.shape[1] // 2), g.dtype) for g in grads]
    scratch += [V((g.shape[0], g.shape[1] // 2), g.dtype) for g in grads]
    scratch += [V((3, F, g.shape[0] // QUAD // F, g.shape[1] // 2), g.dtype) for g in grads]
    scratch += [V((g.shape[0] // QUAD, g.shape[1] // 2), g.dtype) for g in grads]
    scratch += [V((F - 1, g.shape[0] // QUAD // F, g.shape[1] // 2), g.dtype) for g in grads]
    scratch += [V((g.shape[0] // QUAD // F, g.shape[1] // 2), g.dtype) for g in grads]
    if groups > 1:
        scratch += [V((groups - 1, g.shape[0] // QUAD // F, g.shape[1] // 2), g.dtype) for g in grads]
    scratch += [DMA((count,))] * 4 + [DMA((weights,))] * 2 + [DMA((weights, F, 3))] * 2
    scratch += [DMA((weights, F))] * 2 + [DMA((weights, max(groups, 2)))] * 2
    scratch += [DMA((weights, QUAD))] * 2 + [DMA((weights,))] * 2 + [DMA((2 + weights,))]
    return pl.pallas_call(
        functools.partial(reduce_kernel, rep_size, fsdp_size, weights),
        out_shape=outs,
        in_specs=[anywhere] * (2 + weights),
        out_specs=[anywhere] * (2 + weights),
        scratch_shapes=scratch,
        compiler_params=pltpu.CompilerParams(
            collective_id=2, has_side_effects=True, vmem_limit_bytes=56 * 2**20
        ),
        name="reduce_all",
    )(res, gin, *grads)


def widen_kernel(count, *refs):
    for k in range(count):
        refs[count + k][...] = refs[k][...].astype(jnp.float32)


def widen(arrays):
    steps = 4

    def spec(a):
        return pl.BlockSpec((a.shape[0] // steps, a.shape[1]), lambda i: (i, 0))

    return pl.pallas_call(
        functools.partial(widen_kernel, len(arrays)),
        grid=(steps,),
        in_specs=[spec(a) for a in arrays],
        out_specs=[spec(a) for a in arrays],
        out_shape=[jax.ShapeDtypeStruct(a.shape, jnp.float32) for a in arrays],
        name="widen",
    )(*arrays)


def matmul(left, right):
    return jnp.dot(left, right, preferred_element_type=jnp.float32)


def matmul_left_t(left, right):
    return lax.dot_general(
        left, right, (((0,), (0,)), ((), ())), preferred_element_type=jnp.float32
    )


def matmul_right_t(left, right):
    return lax.dot_general(
        left, right, (((1,), (1,)), ((), ())), preferred_element_type=jnp.float32
    )


def norm_backward(grad_out, normed, scaled_inv, norm_gain):
    grad_normed = grad_out * norm_gain
    first_mean = jnp.mean(grad_normed, axis=-1, keepdims=True)
    second_mean = jnp.mean(grad_normed * normed, axis=-1, keepdims=True)
    return (grad_normed - first_mean - normed * second_mean) * scaled_inv


def shards(
    tokens,
    cotangent,
    lengths,
    slot_seq,
    query_weight,
    query_bias,
    key_weight,
    value_weight,
    value_bias,
    out_weight,
    out_bias,
    first_gain,
    first_shift,
    inner_weight,
    inner_bias,
    outer_weight,
    outer_bias,
    second_gain,
    second_shift,
):
    rep_size, fsdp_size = lax.axis_size("rep"), lax.axis_size("fsdp")
    me = lax.axis_index("rep") * fsdp_size + lax.axis_index("fsdp")
    row_count, feature_dim = tokens.shape
    small = [query_bias, value_bias, out_bias, first_gain, first_shift, outer_bias, second_gain, second_shift]
    width = query_bias.shape[0]
    wide = inner_bias.shape[0] // width
    lanes = 256
    vec_rows = 16
    chosen = jnp.arange(fsdp_size, dtype=jnp.int32) == lax.axis_index("fsdp")

    def own_lanes(v):
        return jnp.where(chosen[:, None], v[None, :], jnp.zeros_like(v)[None, :]).reshape(-1)

    last = jnp.pad(inner_bias, (0, max(0, feature_dim - inner_bias.shape[0])))
    vec = jnp.pad(jnp.stack([own_lanes(v) for v in small] + [last]), ((0, vec_rows - 9), (0, 0)))
    length_block = jnp.broadcast_to(lengths.reshape(1, 1), (8, 128))
    (
        seq_rows, seq_seed, all_vec,
        query_full, key_full, value_full, out_full, inner_full, outer_full,
        query_rows, key_rows, value_rows, probs, context, first_normed, first_inv, hidden_low,
        activated, slope, second_normed, second_inv, result, kept_table, _,
    ) = fetch(
        rep_size, fsdp_size, slot_seq, tokens, cotangent, length_block, vec,
        [query_weight, key_weight, value_weight, out_weight, inner_weight, outer_weight],
    )
    kept = kept_table[0] > 0
    params = all_vec.reshape(fsdp_size, vec_rows, feature_dim)[:, :8].astype(jnp.float32).sum(axis=0)
    first_gain_full, second_gain_full = params[3], params[6]
    first_inv, second_inv = first_inv[:, :1], second_inv[:, :1]
    head_shape = (row_count, HEADS, HD)
    seed_rows = jnp.where(kept[:, None], seq_seed.astype(jnp.float32), 0.0)
    grad_second_gain = jnp.sum(seed_rows * second_normed, axis=0)
    grad_second_shift = jnp.sum(seed_rows, axis=0)
    grad_second = norm_backward(seed_rows, second_normed, second_inv, second_gain_full)
    grad_outer = grad_second.astype(jnp.bfloat16)
    grad_outer_bias = jnp.sum(grad_outer, axis=0, dtype=jnp.float32)
    grad_outer_weight = matmul_left_t(activated, grad_outer)
    grad_activated = matmul_right_t(grad_outer, outer_full)
    grad_inner = (grad_activated * slope).astype(jnp.bfloat16)
    grad_inner_bias = jnp.sum(grad_inner, axis=0, dtype=jnp.float32)
    grad_inner_weight = matmul_left_t(hidden_low, grad_inner)
    grad_hidden = grad_second + matmul_right_t(grad_inner, inner_full)
    grad_first_gain = jnp.sum(grad_hidden * first_normed, axis=0)
    grad_first_shift = jnp.sum(grad_hidden, axis=0)
    grad_residual = norm_backward(grad_hidden, first_normed, first_inv, first_gain_full)
    grad_attended = grad_residual.astype(jnp.bfloat16)
    grad_out_bias = jnp.sum(grad_attended, axis=0, dtype=jnp.float32)
    grad_out_weight = matmul_left_t(context, grad_attended)
    grad_context = matmul_right_t(grad_attended, out_full).astype(jnp.bfloat16)
    heads_of = lambda a: a.reshape(head_shape)
    grad_rows_h = heads_of(grad_context)
    prob32 = probs.astype(jnp.float32)
    grad_prob = jnp.einsum(
        "qhd,khd->hqk", grad_rows_h, heads_of(value_rows), preferred_element_type=jnp.float32
    )
    centered = jnp.sum(prob32 * grad_prob, axis=-1, keepdims=True)
    grad_scores = (prob32 * (grad_prob - centered)).astype(jnp.bfloat16)
    back = lambda eq, a, b, scale: (
        (jnp.einsum(eq, a, b, preferred_element_type=jnp.float32) * scale)
        .astype(jnp.bfloat16).reshape(row_count, feature_dim)
    )
    scale = HD ** (-0.5)
    grad_query = back("hqk,khd->qhd", grad_scores, heads_of(key_rows), scale)
    grad_key = back("hqk,qhd->khd", grad_scores, heads_of(query_rows), scale)
    grad_value = back("hqk,qhd->khd", probs, grad_rows_h, 1.0)
    grad_query_bias = jnp.sum(grad_query, axis=0, dtype=jnp.float32)
    grad_value_bias = jnp.sum(grad_value, axis=0, dtype=jnp.float32)
    grad_query_weight = matmul_left_t(seq_rows, grad_query)
    grad_key_weight = matmul_left_t(seq_rows, grad_key)
    grad_value_weight = matmul_left_t(seq_rows, grad_value)
    grad_input = (
        grad_residual
        + matmul_right_t(grad_query, query_full)
        + matmul_right_t(grad_key, key_full)
        + matmul_right_t(grad_value, value_full)
    ).astype(jnp.bfloat16)
    low = lambda g: g.astype(jnp.bfloat16)
    grad_small = [
        grad_query_bias, grad_value_bias, grad_out_bias, grad_first_gain, grad_first_shift,
        grad_outer_bias, grad_second_gain, grad_second_shift,
    ]
    grad_table = jnp.concatenate(
        [
            jnp.stack(grad_small).reshape(8, fsdp_size, width).transpose(1, 0, 2),
            grad_inner_bias.reshape(fsdp_size, wide, width),
        ],
        axis=1,
    )
    grad_rows = 32
    grad_table = jnp.pad(
        grad_table, ((0, 0), (0, grad_rows - 8 - wide), (0, lanes - width))
    ).reshape(fsdp_size * grad_rows, lanes)
    (
        back_rows, back_grads, d_outer, d_inner, d_out, d_query, d_key, d_value, d_vec,
    ) = reduce_all(
        rep_size, fsdp_size, result, grad_input,
        [
            low(grad_outer_weight), low(grad_inner_weight), low(grad_out_weight),
            low(grad_query_weight), low(grad_key_weight), low(grad_value_weight), grad_table,
        ],
    )
    d_outer, d_inner, d_out, d_query, d_key, d_value = widen(
        [d_outer, d_inner, d_out, d_query, d_key, d_value]
    )
    v = d_vec[:, :width]
    return (
        back_rows, back_grads,
        d_query, v[0], d_key, d_value, v[1], d_out, v[2], v[3], v[4],
        d_inner, v[8 : 8 + wide].reshape(-1), d_outer, v[5], v[6], v[7],
    )


def solution(mesh):
    placed = (
        P(("rep", "fsdp"), None),
        P(("rep", "fsdp"), None),
        P(("rep", "fsdp")),
        P(),
        P("fsdp", None),
        P("fsdp"),
        P("fsdp", None),
        P("fsdp", None),
        P("fsdp"),
        P("fsdp", None),
        P("fsdp"),
        P("fsdp"),
        P("fsdp"),
        P("fsdp", None),
        P("fsdp"),
        P("fsdp", None),
        P("fsdp"),
        P("fsdp"),
        P("fsdp"),
    )
    return jax.shard_map(
        shards,
        mesh=mesh,
        in_specs=placed,
        out_specs=(
            P(("rep", "fsdp"), None),
            P(("rep", "fsdp"), None),
            P("fsdp", None),
            P("fsdp"),
            P("fsdp", None),
            P("fsdp", None),
            P("fsdp"),
            P("fsdp", None),
            P("fsdp"),
            P("fsdp"),
            P("fsdp"),
            P("fsdp", None),
            P("fsdp"),
            P("fsdp", None),
            P("fsdp"),
            P("fsdp"),
            P("fsdp"),
        ),
        check_vma=False,
    )
```

```python
import functools

import jax
import jax.numpy as jnp
from jax import lax
from jax.experimental import pallas as pl
from jax.experimental.pallas import tpu as pltpu
from jax.sharding import PartitionSpec as P

HEADS = 12
HD = 64
MESH = pl.DeviceIdType.MESH
DMA = pltpu.SemaphoreType.DMA
QUAD = 4
SAVED = 14


norm_eps = 1e-12
masked_score = -1e30
inv_root_two = 0.7071067811865476
inv_root_two_pi = 0.3989422804014327


def remote(src, dst, send, recv, device):
    return pltpu.make_async_remote_copy(
        src_ref=src, dst_ref=dst, send_sem=send, recv_sem=recv,
        device_id=device, device_id_type=MESH,
    )


def place(linear, fsdp_size):
    return {"rep": lax.div(linear, fsdp_size), "fsdp": lax.rem(linear, fsdp_size)}


def enter(count, fsdp_size, me):
    sem = pltpu.get_barrier_semaphore()

    def greet(k, carry):
        pl.semaphore_signal(
            sem, inc=1, device_id=place(lax.rem(me + k, count), fsdp_size), device_id_type=MESH
        )
        return carry

    lax.fori_loop(1, count, greet, 0)
    pl.semaphore_wait(sem, count - 1)


class Exchange:
    def __init__(self, count, fsdp_size, me, src, dst, rows, sems, spread=False):
        self.args = (count, fsdp_size, me, src, dst, rows, sems, spread)

    def copy(self, k, arriving):
        count, fsdp_size, me, src, dst, rows, (send, recv), spread = self.args
        peer = lax.rem(me + k, count)
        slot = lax.rem(me + count - k, count) if arriving else me
        source = src if spread else src.at[pl.ds(pl.multiple_of(peer * rows, rows), rows)]
        return remote(
            source, dst.at[pl.ds(pl.multiple_of(slot * rows, rows), rows)],
            send.at[k], recv.at[k], place(peer, fsdp_size),
        )

    def start(self):
        def go(k, carry):
            self.copy(k, False).start()
            return carry

        lax.fori_loop(1, self.args[0], go, 0)

    def wait(self):
        def go(k, carry):
            self.copy(k, True).wait()
            return carry

        lax.fori_loop(1, self.args[0], go, 0)


def block_of(ref, index, rows):
    return ref.at[pl.ds(pl.multiple_of(index * rows, rows), rows)]


def position(fsdp_size):
    r = lax.axis_index("rep")
    f = lax.axis_index("fsdp")
    core = lax.rem(r, 2)
    chip = lax.div(r, 2)
    q = lax.rem(chip, QUAD)
    return r, f, core, chip, q, chip - q


def flip(q, bit):
    return q + bit - 2 * bit * lax.rem(lax.div(q, bit), 2)


def fetch_kernel(rep_size, fsdp_size, weights, *refs):
    F = fsdp_size
    refs = list(refs)
    take = lambda k: [refs.pop(0) for _ in range(k)]
    slots, tok, cot, length, vec = take(5)
    shard = take(weights)
    otok, ocot, ovec = take(3)
    full = take(weights)
    saved = take(SAVED)
    olen = take(1)[0]
    stage = take(weights)
    held = take(weights)
    x_v, len_v, vec_v, par_v = take(4)
    keep = take(SAVED)
    load_sem, save_sem = take(2)
    (query_v, key_v, value_v, prob_v, context_v, norm1_v, inv1_v, low_v, act_v, slope_v, norm2_v,
     inv2_v, result_v, keptv) = keep
    xs, xr, ys, yr, ls, lr, vs, vr, zs, zr, qs, qr, ps, pr, own = take(15)
    r, f, core, chip, q, base = position(F)
    count = rep_size * F
    me = r * F + f
    rows = tok.shape[0] // count
    vrows = vec.shape[0]
    lrows = length.shape[0]
    enter(count, F, me)

    trade_tok = Exchange(count, F, me, tok, otok, rows, (xs, xr))
    trade_cot = Exchange(count, F, me, cot, ocot, rows, (ys, yr))
    trade_len = Exchange(count, F, me, length, olen, lrows, (ls, lr), spread=True)

    def piece(ref, w, shard_row, quarter):
        S, C = shard[w].shape
        sq, half = S // QUAD, C // 2
        return ref.at[
            pl.ds(pl.multiple_of(shard_row * S + quarter * sq, sq), sq),
            pl.ds(pl.multiple_of(core * half, half), half),
        ]

    def strip(w, shard_row, which):
        S, C = shard[w].shape
        half = C // 2
        return full[w].at[
            pl.ds(pl.multiple_of(shard_row * S, S), S), pl.ds(pl.multiple_of(which * half, half), half)
        ]

    near = (flip(q, 1), flip(q, 2))
    far = flip(near[0], 2)

    def chip_at(quarter):
        return {"rep": (base + quarter) * 2 + core, "fsdp": f}

    partner = {"rep": chip * 2 + (1 - core), "fsdp": f}

    def along(w, row, step):
        source = piece(full[w], w, row, q)
        return remote(
            source, source, zs.at[w, row, (1 - step) // 2], zr.at[w, row], {"rep": r, "fsdp": f + step}
        )

    def first_along(w, step):
        return remote(
            piece(shard[w], w, 0, q), piece(full[w], w, f, q),
            zs.at[w, f, (1 - step) // 2], zr.at[w, f], {"rep": r, "fsdp": f + step},
        )

    def across(w, row, side, arriving):
        part = piece(full[w], w, row, near[side] if arriving else q)
        return remote(part, part, qs.at[w, row, side], qr.at[w, row, side], chip_at(near[side]))

    def relay(w, row, arriving):
        turn = lax.rem(row + w, 2)
        part = piece(full[w], w, row, far if arriving else jnp.where(turn == 0, near[1], near[0]))
        to = chip_at(jnp.where(turn == 0, near[0], near[1]))
        return remote(part, part, qs.at[w, row, 2], qr.at[w, row, 2], to)

    def beside(w, j, arriving):
        row = lax.rem(f + j, F)
        part = strip(w, row, (1 - core) if arriving else core)
        return remote(part, part, ps.at[w, j], pr.at[w, j], partner)

    def vector(j, arriving):
        to = lax.rem(f + j, F)
        row = lax.rem(f + F - j, F) if arriving else f
        return remote(vec, block_of(ovec, row, vrows), vs.at[j], vr.at[j], {"rep": r, "fsdp": to})

    trade_len.start()
    for j in range(1, F):
        vector(j, False).start()
    trade_tok.start()
    for w in range(weights):
        @pl.when(f < F - 1)
        def _():
            first_along(w, 1).start()

        @pl.when(f > 0)
        def _():
            first_along(w, -1).start()

    local = [
        pltpu.make_async_copy(block_of(tok, me, rows), block_of(otok, me, rows), own.at[0]),
        pltpu.make_async_copy(block_of(cot, me, rows), block_of(ocot, me, rows), own.at[1]),
        pltpu.make_async_copy(length, block_of(olen, me, lrows), own.at[2]),
        pltpu.make_async_copy(vec, block_of(ovec, f, vrows), own.at[3]),
    ]
    into = [pltpu.make_async_copy(shard[w], stage[w], own.at[4 + w]) for w in range(weights)]
    for c in local + into:
        c.start()
    out = []
    for w in range(weights):
        into[w].wait()
        c = pltpu.make_async_copy(stage[w], block_of(full[w], f, shard[w].shape[0]), own.at[4 + w])
        c.start()
        out.append(c)

    def step_two(w):
        for d in range(1, F):
            for step in (1, -1):
                row = f - d * step

                @pl.when((row >= 0) & (row < F))
                def _():
                    along(w, row, step).wait_recv()

                    @pl.when((f + step >= 0) & (f + step < F))
                    def _():
                        along(w, row, step).start()

                    across(w, row, 0, False).start()
                    across(w, row, 1, False).start()

    def step_turn(w):
        for j in range(1, F):
            row = lax.rem(f + j, F)
            across(w, row, 0, True).wait_recv()
            across(w, row, 1, True).wait_recv()
            relay(w, row, False).start()

    def step_three(w):
        for j in range(1, F):
            relay(w, lax.rem(f + j, F), True).wait_recv()
            beside(w, j, False).start()

    def step_four(w):
        for j in range(1, F):
            beside(w, j, True).wait_recv()

    steps = (step_two, step_turn, step_three, step_four)

    def advance(at):
        for k, step in enumerate(steps):
            if 0 <= at - k < weights:
                step(at - k)
        done = at - len(steps) + 1
        if 0 <= done < weights:
            out[done].wait()
            pltpu.make_async_copy(full[done], held[done], load_sem.at[done]).start()

    def ready(w):
        pltpu.make_async_copy(full[w], held[w], load_sem.at[w]).wait()

    def store(k):
        pltpu.make_async_copy(keep[k], saved[k], save_sem.at[k]).start()

    n_rows, width = x_v.shape
    f32, bf16 = jnp.float32, jnp.bfloat16

    def project(dst, w, bias):
        tile = 256

        def go(i, carry):
            at = pl.ds(pl.multiple_of(i * tile, tile), tile)
            total = jnp.dot(x_v[...], held[w][:, at], preferred_element_type=f32)
            if bias is not None:
                total = total + par_v[bias : bias + 1, at]
            dst[:, at] = total.astype(bf16)
            return carry

        lax.fori_loop(0, width // tile, go, 0)

    def attend(first, last):
        block = 256
        blocks = n_rows // block

        def go(i, carry):
            pair = lax.div(i, blocks)
            rows_at = pl.ds(pl.multiple_of(lax.rem(i, blocks) * block, block), block)
            lanes = pl.ds(pl.multiple_of(pair * 128, 128), 128)
            lane = lax.broadcasted_iota(jnp.int32, (n_rows, 128), 1)
            queries = query_v[rows_at, lanes]
            keys = key_v[:, lanes]
            values = value_v[:, lanes]
            seen = keptv[0:1, :]
            total = jnp.zeros((block, 128), f32)
            for side in range(2):
                mine = (lane >= side * HD) & (lane < side * HD + HD)
                k_side = jnp.where(mine, keys, jnp.zeros_like(keys))
                v_side = jnp.where(mine, values, jnp.zeros_like(values))
                scores = matmul_right_t(queries, k_side) * HD ** (-0.5)
                scores = jnp.where(seen > 0, scores, masked_score)
                largest = jnp.max(scores, axis=-1, keepdims=True)
                powers = jnp.exp(scores - largest)
                probs = (powers * (1.0 / jnp.sum(powers, axis=-1, keepdims=True))).astype(bf16)
                prob_v[pair * 2 + side, rows_at, :] = probs
                total = total + jnp.dot(probs, v_side, preferred_element_type=f32)
            context_v[rows_at, lanes] = total.astype(bf16)
            return carry

        lax.fori_loop(first * blocks, last * blocks, go, 0)

    def normalize(values):
        center = values - jnp.mean(values, axis=-1, keepdims=True)
        inv = lax.rsqrt(jnp.mean(center * center, axis=-1, keepdims=True) + norm_eps)
        return center * inv, inv

    def first_half():
        block = 128

        def go(i, carry):
            at = pl.ds(pl.multiple_of(i * block, block), block)
            total = jnp.dot(context_v[at, :], held[3][...], preferred_element_type=f32)
            normed, inv = normalize(x_v[at, :].astype(f32) + (total + par_v[2:3, :width]))
            norm1_v[at, :] = normed
            inv1_v[at, :] = jnp.broadcast_to(inv, (block, 128))
            low_v[at, :] = (normed * par_v[3:4, :width] + par_v[4:5, :width]).astype(bf16)
            return carry

        lax.fori_loop(0, n_rows // block, go, 0)

    def widen_out(first, last):
        tile = 256

        def go(i, carry):
            at = pl.ds(pl.multiple_of(i * tile, tile), tile)
            block = 256

            def rows_go(k, c2):
                rows_at = pl.ds(pl.multiple_of(k * block, block), block)
                inner = jnp.dot(low_v[rows_at, :], held[4][:, at], preferred_element_type=f32)
                inner = inner + par_v[8:9, at]
                share = 0.5 * (1.0 + lax.erf(inner * inv_root_two))
                act_v[rows_at, at] = (inner * share).astype(bf16)
                slope = share + inner * jnp.exp(-0.5 * inner * inner) * inv_root_two_pi
                slope_v[rows_at, at] = slope.astype(bf16)
                return c2

            lax.fori_loop(0, n_rows // block, rows_go, 0)
            return carry

        lax.fori_loop(first, last, go, 0)

    def second_half():
        block = 128

        def go(i, carry):
            at = pl.ds(pl.multiple_of(i * block, block), block)
            total = jnp.dot(act_v[at, :], held[5][...], preferred_element_type=f32)
            hidden = norm1_v[at, :] * par_v[3:4, :width] + par_v[4:5, :width]
            normed, inv = normalize(hidden + (total + par_v[5:6, :width]))
            norm2_v[at, :] = normed
            inv2_v[at, :] = jnp.broadcast_to(inv, (block, 128))
            row = lax.broadcasted_iota(jnp.int32, (block, 1), 0) + i * block
            live = row < jnp.max(keptv[1:2, 0:1])
            result = normed * par_v[6:7, :width] + par_v[7:8, :width]
            result_v[at, :] = jnp.where(live, result, 0.0).astype(bf16)
            return carry

        lax.fori_loop(0, n_rows // block, go, 0)
        for k in (10, 11, 12):
            store(k)

    advance(0)
    advance(1)
    advance(2)
    for j in range(1, F):
        vector(j, True).wait()
    trade_len.wait()
    trade_tok.wait()
    for c in local:
        c.wait()
    fill = [
        pltpu.make_async_copy(otok, x_v, load_sem.at[weights]),
        pltpu.make_async_copy(olen, len_v, load_sem.at[weights + 1]),
        pltpu.make_async_copy(ovec, vec_v, load_sem.at[weights + 2]),
    ]
    for c in fill:
        c.start()
    for c in fill:
        c.wait()
    narrow = jnp.zeros((8, width), f32)
    for k in range(F):
        narrow = narrow + vec_v[k * vrows : k * vrows + 16, :].astype(f32)[0:8, :]
    par_v[0:8, 0:width] = narrow
    part = shard[5].shape[0]
    for k in range(F):
        par_v[8:9, k * part : (k + 1) * part] = vec_v[k * vrows : k * vrows + 16, :].astype(f32)[8:9, 0:part]
    mine = slots[me]
    owner = lax.div(lax.broadcasted_iota(jnp.int32, len_v.shape, 0), lrows)
    my_length = jnp.max(jnp.where(owner == mine, len_v[...], 0))
    key_at = lax.broadcasted_iota(jnp.int32, (8, n_rows), 1)
    second = lax.broadcasted_iota(jnp.int32, (8, n_rows), 0) > 0
    keptv[...] = jnp.where(second, my_length, (key_at < my_length).astype(jnp.int32))
    advance(3)
    ready(0)
    project(query_v, 0, 0)
    advance(4)
    ready(1)
    project(key_v, 1, None)
    advance(5)
    trade_cot.start()
    ready(2)
    project(value_v, 2, 1)
    for k in (0, 1, 2):
        store(k)
    attend(0, 2)
    advance(6)
    attend(2, 4)
    advance(7)
    attend(4, 6)
    for k in (3, 4):
        store(k)
    ready(3)
    first_half()
    for k in (5, 6, 7):
        store(k)
    tiles = held[4].shape[1] // 256
    ready(4)
    widen_out(0, tiles // 2)
    advance(8)
    widen_out(tiles // 2, tiles)
    for k in (8, 9):
        store(k)
    ready(5)
    second_half()
    store(13)
    for w in range(weights):
        for step in (1, -1):

            @pl.when((f + step >= 0) & (f + step < F))
            def _():
                first_along(w, step).wait_send()
                for d in range(1, F):
                    row = f - d * step

                    @pl.when((row >= 0) & (row < F))
                    def _():
                        along(w, row, step).wait_send()

        for j in range(1, F):
            row = lax.rem(f + j, F)
            across(w, row, 0, False).wait_send()
            across(w, row, 1, False).wait_send()
            relay(w, row, False).wait_send()
            beside(w, j, False).wait_send()
    trade_cot.wait()
    for k in range(SAVED):
        pltpu.make_async_copy(keep[k], saved[k], save_sem.at[k]).wait()


def fetch(rep_size, fsdp_size, slots, tok, cot, length, vec, shards_in):
    weights = len(shards_in)
    count = rep_size * fsdp_size
    F = fsdp_size
    like = jax.ShapeDtypeStruct
    n_rows, width = tok.shape
    hidden_width = shards_in[4].shape[1]
    bf16, f32 = jnp.bfloat16, jnp.float32
    rows_of = lambda columns, kind: like((n_rows, columns), kind)
    save = [rows_of(width, bf16)] * 3 + [like((HEADS, n_rows, n_rows), bf16), rows_of(width, bf16)]
    save += [rows_of(width, f32), rows_of(128, f32), rows_of(width, bf16)]
    save += [rows_of(hidden_width, bf16)] * 2 + [rows_of(width, f32), rows_of(128, f32), rows_of(width, bf16)]
    save += [like((8, n_rows), jnp.int32)]
    wide = [like((w.shape[0] * F, w.shape[1]), w.dtype) for w in shards_in]
    outs = [
        like(tok.shape, tok.dtype), like(cot.shape, cot.dtype),
        like((F * vec.shape[0], vec.shape[1]), vec.dtype),
    ] + wide + save + [like((count * length.shape[0], length.shape[1]), length.dtype)]
    anywhere = pl.BlockSpec(memory_space=pl.ANY)
    V = lambda a: pltpu.VMEM(a.shape, a.dtype)
    return pl.pallas_call(
        functools.partial(fetch_kernel, rep_size, fsdp_size, weights),
        out_shape=outs,
        in_specs=[pl.BlockSpec(memory_space=pltpu.SMEM)] + [anywhere] * (4 + weights),
        out_specs=[anywhere] * len(outs),
        scratch_shapes=[V(w) for w in shards_in]
        + [V(w) for w in wide]
        + [V(tok), V(outs[-1]), V(outs[2]), pltpu.VMEM((16, hidden_width), f32)]
        + [V(a) for a in save]
        + [DMA((weights + 3,)), DMA((SAVED,))]
        + [DMA((count,))] * 6
        + [DMA((F,))] * 2
        + [DMA((weights, F, 2)), DMA((weights, F))]
        + [DMA((weights, F, 3))] * 2
        + [DMA((weights, F))] * 2
        + [DMA((4 + weights,))],
        compiler_params=pltpu.CompilerParams(
            collective_id=1, has_side_effects=True, vmem_limit_bytes=60 * 2**20
        ),
        name="forward",
    )(slots, tok, cot, length, vec, *shards_in)


LOADED = 17


def backward_kernel(rep_size, fsdp_size, weights, *refs):
    F = fsdp_size
    refs = list(refs)
    take = lambda k: [refs.pop(0) for _ in range(k)]
    res, prob = take(2)
    given = take(LOADED)
    inv1, inv2, kept_in, vec_in = take(4)
    ores, ogin, gin = take(3)
    owned = take(weights)
    have = take(LOADED)
    (w_outer, w_inner, w_out, w_query, w_key, w_value, x_v, seed_v, query_v, key_v, value_v,
     context_v, norm1_v, norm2_v, low_v, act_v, slope_v) = have
    inv1_v, inv2_v, kept_v, vec_v, par_v = take(5)
    prob_v, gf_v, ga_v, gc_v, gq_v, gk_v, gv_v, gin_v, sum_v, sum_in_v, table_v = take(11)
    half_in = take(weights)
    half_out = take(weights)
    quad_in = take(weights)
    quad_sum = take(weights)
    line_in = take(weights)
    line_sum = take(weights)
    group_count = rep_size // (2 * QUAD)
    group_in = take(weights) if group_count > 1 else None
    xs, xr, ys, yr, ps, pr, qs, qr, zs, zr, gs, gr, hs, hr, bs, br, own, load_sem, prob_sem = take(19)
    r, f, core, chip, q, base = position(F)
    count = rep_size * F
    me = r * F + f
    rows = res.shape[0] // count
    enter(count, F, me)

    trade_res = Exchange(count, F, me, res, ores, rows, (xs, xr))
    trade_gin = Exchange(count, F, me, gin, ogin, rows, (ys, yr))
    partner = {"rep": chip * 2 + (1 - core), "fsdp": f}

    def mate(m):
        return {"rep": (base + lax.rem(q + m, QUAD)) * 2 + core, "fsdp": f}

    def columns(ref, w, which):
        half = half_in[w].shape[1]
        return ref.at[:, pl.ds(pl.multiple_of(which * half, half), half)]

    def swap(w):
        return remote(half_out[w], half_in[w], ps.at[w], pr.at[w], partner)

    def size(w):
        S = half_in[w].shape[0] // F
        return S, S // QUAD

    near = (flip(q, 1), flip(q, 2))
    far = flip(near[0], 2)

    def chip_at(quarter):
        return {"rep": (base + quarter) * 2 + core, "fsdp": f}

    def rows_of(w, t, quarter):
        S, sq = size(w)
        return pl.ds(pl.multiple_of(t * S + quarter * sq, sq), sq)

    def across(w, t, k):
        side = (w + t) % 2
        return remote(
            half_in[w].at[rows_of(w, t, (near[side], far)[k])], quad_in[w].at[k, t],
            qs.at[w, t, k], qr.at[w, t, k], chip_at(near[side]),
        )

    def turn(w, t):
        side = 1 - (w + t) % 2
        return remote(
            half_in[w].at[rows_of(w, t, near[side])], quad_in[w].at[2, t],
            qs.at[w, t, 2], qr.at[w, t, 2], chip_at(near[side]),
        )

    def along(w, j):
        S, sq = size(w)
        to = lax.rem(f + j, F)
        return remote(
            quad_sum[w].at[pl.ds(pl.multiple_of(to * sq, sq), sq)], line_in[w].at[j - 1],
            zs.at[w, j], zr.at[w, j], {"rep": r, "fsdp": to},
        )

    def group(w, g):
        to = lax.rem(lax.div(chip, QUAD) + g, group_count)
        return remote(
            line_sum[w], group_in[w].at[g - 1], gs.at[w, g], gr.at[w, g],
            {"rep": (to * QUAD + q) * 2 + core, "fsdp": f},
        )

    def home(w, quarter, which):
        S, sq = size(w)
        half = half_in[w].shape[1]
        return owned[w].at[
            pl.ds(pl.multiple_of(quarter * sq, sq), sq), pl.ds(pl.multiple_of(which * half, half), half)
        ]

    def spread(w, m, arriving):
        S, sq = size(w)
        return remote(
            line_sum[w], home(w, lax.rem(q + QUAD - m, QUAD) if arriving else q, core),
            hs.at[w, m], hr.at[w, m], mate(m),
        )

    def beside(w, arriving):
        part = columns(owned[w], w, (1 - core) if arriving else core)
        return remote(part, part, bs.at[w], br.at[w], partner)

    f32, bf16 = jnp.float32, jnp.bfloat16
    n_rows, width = x_v.shape
    wide = slope_v.shape[1]
    sources = [
        (act_v, gf_v), (low_v, slope_v), (context_v, ga_v), (x_v, gq_v), (x_v, gk_v), (x_v, gv_v)
    ]
    table_at = weights - 1

    def load(k):
        return pltpu.make_async_copy(given[k], have[k], load_sem.at[k])

    def gradient(w, which, emit):
        if w == table_at:
            emit(pl.ds(0, table_v.shape[0]), pl.ds(0, 128),
                 table_v[:, pl.ds(pl.multiple_of(which * 128, 128), 128)])
            return
        left, right = sources[w]
        half = half_in[w].shape[1]
        tile = 256
        span = min(half, 768)
        across_tiles = half // span

        def go(i, carry):
            rows_at = pl.ds(pl.multiple_of(lax.div(i, across_tiles) * tile, tile), tile)
            start = lax.rem(i, across_tiles) * span
            from_at = pl.ds(pl.multiple_of(which * half + start, 128), span)
            total = matmul_left_t(left[:, rows_at], right[:, from_at])
            emit(rows_at, pl.ds(pl.multiple_of(start, 128), span), total)
            return carry

        lax.fori_loop(0, left.shape[1] // tile * across_tiles, go, 0)

    def offer(w):
        def emit(rows_at, cols_at, total):
            half_out[w][rows_at, cols_at] = total.astype(half_out[w].dtype)

        gradient(w, 1 - core, emit)
        swap(w).start()

    def step_one(w):
        swap(w).wait_recv()

        def emit(rows_at, cols_at, total):
            total = total + half_in[w][rows_at, cols_at].astype(f32)
            half_in[w][rows_at, cols_at] = total.astype(half_in[w].dtype)

        gradient(w, core, emit)
        for t in range(F):
            for k in range(2):
                across(w, t, k).start()

    def step_turn(w):
        for t in range(F):
            for k in range(2):
                across(w, t, k).wait_recv()
            at = rows_of(w, t, near[1 - (w + t) % 2])
            total = half_in[w][at, :].astype(jnp.float32) + quad_in[w][1, t].astype(jnp.float32)
            half_in[w][at, :] = total.astype(half_in[w].dtype)
            turn(w, t).start()

    def step_two(w):
        S, sq = size(w)
        for t in range(F):
            turn(w, t).wait_recv()
            total = half_in[w][rows_of(w, t, q), :].astype(jnp.float32)
            total = total + quad_in[w][0, t].astype(jnp.float32) + quad_in[w][2, t].astype(jnp.float32)
            quad_sum[w][pl.ds(t * sq, sq), :] = total.astype(quad_sum[w].dtype)
        for j in range(1, F):
            along(w, j).start()

    def step_three(w):
        S, sq = size(w)
        for j in range(1, F):
            along(w, j).wait_recv()
        total = quad_sum[w][pl.ds(pl.multiple_of(f * sq, sq), sq), :].astype(jnp.float32)
        for j in range(F - 1):
            total = total + line_in[w][j].astype(jnp.float32)
        line_sum[w][...] = total.astype(line_sum[w].dtype)
        for g in range(1, group_count):
            group(w, g).start()
        if group_count == 1:
            finish(w)

    def step_group(w):
        for g in range(1, group_count):
            group(w, g).wait()
        total = line_sum[w][...].astype(jnp.float32)
        for g in range(group_count - 1):
            total = total + group_in[w][g].astype(jnp.float32)
        line_sum[w][...] = total.astype(line_sum[w].dtype)
        finish(w)

    def finish(w):
        for m in range(1, QUAD):
            spread(w, m, False).start()
        c = pltpu.make_async_copy(line_sum[w], home(w, q, core), own.at[5 + w])
        c.start()
        c.wait()

    def step_four(w):
        for m in range(1, QUAD):
            spread(w, m, True).wait_recv()
        beside(w, False).start()

    row_block = 128
    blocks = n_rows // row_block

    def sum_rows(k, values):
        sum_v[k : k + 1, :] = sum_v[k : k + 1, :] + jnp.sum(values, axis=0, keepdims=True)

    def norm_back(grad_out, normed, inv, gain):
        grad_normed = grad_out * gain
        first = jnp.mean(grad_normed, axis=-1, keepdims=True)
        second = jnp.mean(grad_normed * normed, axis=-1, keepdims=True)
        return (grad_normed - first - normed * second) * inv

    def second_norm():
        def go(i, carry):
            at = pl.ds(pl.multiple_of(i * row_block, row_block), row_block)
            row = lax.broadcasted_iota(jnp.int32, (row_block, 1), 0) + i * row_block
            live = row < jnp.max(kept_v[1:2, 0:1])
            seed = jnp.where(live, seed_v[at, :].astype(f32), 0.0)
            normed = norm2_v[at, :]
            sum_rows(6, seed * normed)
            sum_rows(7, seed)
            grad = norm_back(seed, normed, inv2_v[at, 0:1], par_v[6:7, :])
            norm2_v[at, :] = grad
            low = grad.astype(bf16)
            gf_v[at, :] = low
            sum_rows(5, low.astype(f32))
            return carry

        lax.fori_loop(0, blocks, go, 0)

    def through_gelu():
        tile = 256

        def go(i, carry):
            at = pl.ds(pl.multiple_of(i * tile, tile), tile)
            grad = matmul_right_t(gf_v[...], w_outer[at, :])
            low = (grad * slope_v[:, at].astype(f32)).astype(bf16)
            slope_v[:, at] = low
            sum_in_v[0:1, at] = jnp.sum(low.astype(f32), axis=0, keepdims=True)
            return carry

        lax.fori_loop(0, wide // tile, go, 0)

    def first_norm():
        def go(i, carry):
            at = pl.ds(pl.multiple_of(i * row_block, row_block), row_block)
            grad = norm2_v[at, :] + matmul_right_t(slope_v[at, :], w_inner[...])
            normed = norm1_v[at, :]
            sum_rows(3, grad * normed)
            sum_rows(4, grad)
            grad = norm_back(grad, normed, inv1_v[at, 0:1], par_v[3:4, :])
            norm2_v[at, :] = grad
            low = grad.astype(bf16)
            ga_v[at, :] = low
            sum_rows(2, low.astype(f32))
            return carry

        lax.fori_loop(0, blocks, go, 0)

    def through_out():
        tile = 256

        def go(i, carry):
            at = pl.ds(pl.multiple_of(i * tile, tile), tile)
            gc_v[:, at] = matmul_right_t(ga_v[...], w_out[at, :]).astype(bf16)
            return carry

        lax.fori_loop(0, width // tile, go, 0)

    def prob_load(pair):
        slot = lax.rem(pair, 2)
        return pltpu.make_async_copy(prob.at[pl.ds(pair * 2, 2)], prob_v.at[slot], prob_sem.at[slot])

    pairs = width // 128
    scale = HD ** (-0.5)

    def attend_back(first, last):
        def go(pair, carry):
            prob_load(pair).wait()

            @pl.when(pair + 1 < pairs)
            def _():
                prob_load(pair + 1).start()

            slot = lax.rem(pair, 2)
            lanes = pl.ds(pl.multiple_of(pair * 128, 128), 128)
            block = 256
            lane = lax.broadcasted_iota(jnp.int32, (n_rows, 128), 1)
            keys, values = key_v[:, lanes], value_v[:, lanes]
            zero = jnp.zeros_like(keys)
            grad_key = jnp.zeros((n_rows, 128), f32)
            grad_value = jnp.zeros((n_rows, 128), f32)
            for start in range(0, n_rows, block):
                queries = query_v[start : start + block, lanes]
                grads = gc_v[start : start + block, lanes]
                grad_query = jnp.zeros((block, 128), f32)
                for side in range(2):
                    mine = (lane >= side * HD) & (lane < side * HD + HD)
                    part = mine[:block]
                    chance = prob_v[slot, side, start : start + block, :]
                    wide_chance = chance.astype(f32)
                    grad_prob = matmul_right_t(grads, jnp.where(mine, values, zero))
                    centered = jnp.sum(wide_chance * grad_prob, axis=-1, keepdims=True)
                    grad_score = (wide_chance * (grad_prob - centered)).astype(bf16)
                    grad_query = grad_query + jnp.dot(
                        grad_score, jnp.where(mine, keys, zero), preferred_element_type=f32
                    )
                    grad_key = grad_key + matmul_left_t(
                        grad_score, jnp.where(part, queries, zero[:block])
                    )
                    grad_value = grad_value + matmul_left_t(
                        chance, jnp.where(part, grads, zero[:block])
                    )
                gq_v[start : start + block, lanes] = (grad_query * scale).astype(bf16)
            gk_v[:, lanes] = (grad_key * scale).astype(bf16)
            gv_v[:, lanes] = grad_value.astype(bf16)
            return carry

        lax.fori_loop(first, last, go, 0)

    def input_grad():
        def go(i, carry):
            at = pl.ds(pl.multiple_of(i * row_block, row_block), row_block)
            total = norm2_v[at, :] + matmul_right_t(gq_v[at, :], w_query[...])
            total = total + matmul_right_t(gk_v[at, :], w_key[...])
            total = total + matmul_right_t(gv_v[at, :], w_value[...])
            gin_v[at, :] = total.astype(bf16)
            sum_rows(0, gq_v[at, :].astype(f32))
            sum_rows(1, gv_v[at, :].astype(f32))
            return carry

        lax.fori_loop(0, blocks, go, 0)

    def fill_table():
        table_v[...] = jnp.zeros_like(table_v)
        each = table_v.shape[0] // F
        thin, part = width // F, wide // F
        for t in range(F):
            table_v[t * each : t * each + 8, 0:thin] = sum_v[0:8, :][:, t * thin : (t + 1) * thin]
            for k in range(part // 128):
                table_v[t * each + 8 + k : t * each + 9 + k, 0:128] = (
                    sum_in_v[0:1, t * part + k * 128 : t * part + (k + 1) * 128]
                )

    steps = [step_one, step_turn, step_two, step_three] + ([step_group] if group_count > 1 else []) + [step_four]
    done = [0] * weights

    def run(*ws):
        for w in ws:
            if done[w] < len(steps):
                steps[done[w]](w)
                done[w] += 1

    trade_res.start()
    small = [
        pltpu.make_async_copy(a, b, own.at[1 + k])
        for k, (a, b) in enumerate(
            ((inv1, inv1_v), (inv2, inv2_v), (kept_in, kept_v), (vec_in, vec_v))
        )
    ]
    keep_res = pltpu.make_async_copy(block_of(res, me, rows), block_of(ores, me, rows), own.at[0])
    keep_res.start()
    for c in small:
        c.start()
    for k in (7, 13, 15, 0, 16, 14, 1, 12, 11, 2, 8, 9, 10, 6, 3, 4, 5):
        load(k).start()
    prob_load(0).start()
    sum_v[...] = jnp.zeros_like(sum_v)
    sum_in_v[...] = jnp.zeros_like(sum_in_v)
    for c in small:
        c.wait()
    narrow = jnp.zeros((8, width), f32)
    vrows = vec_v.shape[0] // F
    for k in range(F):
        narrow = narrow + vec_v[k * vrows : k * vrows + 16, :].astype(f32)[0:8, :]
    par_v[...] = narrow
    for k in (7, 13):
        load(k).wait()
    second_norm()
    load(15).wait()
    offer(0)
    for k in (0, 16):
        load(k).wait()
    through_gelu()
    run(0)
    load(14).wait()
    offer(1)
    for k in (1, 12):
        load(k).wait()
    first_norm()
    run(0, 1)
    for k in (11, 2):
        load(k).wait()
    offer(2)
    through_out()
    for k in (8, 9, 10):
        load(k).wait()
    attend_back(0, pairs // 3)
    run(0, 2)
    attend_back(pairs // 3, 2 * pairs // 3)
    run(1, 0)
    attend_back(2 * pairs // 3, pairs)
    load(6).wait()
    for w in (3, 4, 5):
        offer(w)
    run(2, 1)
    for k in (3, 4, 5):
        load(k).wait()
    input_grad()
    put = pltpu.make_async_copy(gin_v, gin, load_sem.at[LOADED])
    put.start()
    fill_table()
    offer(table_at)
    put.wait()
    keep_gin = pltpu.make_async_copy(block_of(gin, me, rows), block_of(ogin, me, rows), own.at[0])
    keep_res.wait()
    trade_gin.start()
    keep_gin.start()
    local = [keep_gin]
    run(3, 4, 5, 6)
    while min(done) < len(steps):
        run(*range(weights))
    for w in range(weights):
        beside(w, True).wait_recv()
        swap(w).wait_send()
        for t in range(F):
            across(w, t, 0).wait_send()
            across(w, t, 1).wait_send()
            turn(w, t).wait_send()
        for m in range(1, QUAD):
            spread(w, m, False).wait_send()
        for j in range(1, F):
            along(w, j).wait_send()
        beside(w, False).wait_send()
    for c in local:
        c.wait()
    trade_res.wait()
    trade_gin.wait()


def backward(rep_size, fsdp_size, res, prob, given, inv1, inv2, kept, vec):
    count = rep_size * fsdp_size
    F = fsdp_size
    groups = rep_size // (2 * QUAD)
    like = jax.ShapeDtypeStruct
    bf16, f32 = jnp.bfloat16, jnp.float32
    anywhere = pl.BlockSpec(memory_space=pl.ANY)
    n_rows, width = res.shape
    grads = [like(w.shape, bf16) for w in given[:6]] + [like((F * 32, 256), f32)]
    weights = len(grads)
    outs = [like(res.shape, res.dtype)] * 3 + [
        like((g.shape[0] // F, g.shape[1]), g.dtype) for g in grads
    ]
    V = pltpu.VMEM
    halves = [(g.shape[0], g.shape[1] // 2, g.dtype) for g in grads]
    rows_of = lambda columns, kind: V((n_rows, columns), kind)
    scratch = [V(a.shape, a.dtype) for a in list(given) + [inv1, inv2, kept, vec]]
    scratch += [V((8, width), f32), V((2, 2, n_rows, n_rows), bf16)]
    scratch += [rows_of(width, bf16)] * 7
    scratch += [V((8, width), f32), V((8, given[1].shape[1]), f32), V((F * 32, 256), f32)]
    scratch += [V((r, c), d) for r, c, d in halves]
    scratch += [V((r, c), d) for r, c, d in halves]
    scratch += [V((3, F, r // QUAD // F, c), d) for r, c, d in halves]
    scratch += [V((r // QUAD, c), d) for r, c, d in halves]
    scratch += [V((F - 1, r // QUAD // F, c), d) for r, c, d in halves]
    scratch += [V((r // QUAD // F, c), d) for r, c, d in halves]
    if groups > 1:
        scratch += [V((groups - 1, r // QUAD // F, c), d) for r, c, d in halves]
    scratch += [DMA((count,))] * 4 + [DMA((weights,))] * 2 + [DMA((weights, F, 3))] * 2
    scratch += [DMA((weights, F))] * 2 + [DMA((weights, max(groups, 2)))] * 2
    scratch += [DMA((weights, QUAD))] * 2 + [DMA((weights,))] * 2 + [DMA((5 + weights,))]
    scratch += [DMA((LOADED + 1,)), DMA((2,))]
    outs_all = pl.pallas_call(
        functools.partial(backward_kernel, rep_size, fsdp_size, weights),
        out_shape=outs,
        in_specs=[anywhere] * (6 + LOADED),
        out_specs=[anywhere] * len(outs),
        scratch_shapes=scratch,
        compiler_params=pltpu.CompilerParams(
            collective_id=2, has_side_effects=True, vmem_limit_bytes=67043328
        ),
        name="backward",
    )(res, prob, *given, inv1, inv2, kept, vec)
    return outs_all[0], outs_all[1], outs_all[3:]


def widen_kernel(count, *refs):
    for k in range(count):
        refs[count + k][...] = refs[k][...].astype(jnp.float32)


def widen(arrays):
    steps = 4

    def spec(a):
        return pl.BlockSpec((a.shape[0] // steps, a.shape[1]), lambda i: (i, 0))

    return pl.pallas_call(
        functools.partial(widen_kernel, len(arrays)),
        grid=(steps,),
        in_specs=[spec(a) for a in arrays],
        out_specs=[spec(a) for a in arrays],
        out_shape=[jax.ShapeDtypeStruct(a.shape, jnp.float32) for a in arrays],
        name="widen",
    )(*arrays)


def matmul(left, right):
    return jnp.dot(left, right, preferred_element_type=jnp.float32)


def matmul_left_t(left, right):
    return lax.dot_general(
        left, right, (((0,), (0,)), ((), ())), preferred_element_type=jnp.float32
    )


def matmul_right_t(left, right):
    return lax.dot_general(
        left, right, (((1,), (1,)), ((), ())), preferred_element_type=jnp.float32
    )


def shards(
    tokens,
    cotangent,
    lengths,
    slot_seq,
    query_weight,
    query_bias,
    key_weight,
    value_weight,
    value_bias,
    out_weight,
    out_bias,
    first_gain,
    first_shift,
    inner_weight,
    inner_bias,
    outer_weight,
    outer_bias,
    second_gain,
    second_shift,
):
    rep_size, fsdp_size = lax.axis_size("rep"), lax.axis_size("fsdp")
    me = lax.axis_index("rep") * fsdp_size + lax.axis_index("fsdp")
    row_count, feature_dim = tokens.shape
    small = [query_bias, value_bias, out_bias, first_gain, first_shift, outer_bias, second_gain, second_shift]
    width = query_bias.shape[0]
    vec_rows = 16
    chosen = jnp.arange(fsdp_size, dtype=jnp.int32) == lax.axis_index("fsdp")

    def own_lanes(v):
        return jnp.where(chosen[:, None], v[None, :], jnp.zeros_like(v)[None, :]).reshape(-1)

    last = jnp.pad(inner_bias, (0, max(0, feature_dim - inner_bias.shape[0])))
    vec = jnp.pad(jnp.stack([own_lanes(v) for v in small] + [last]), ((0, vec_rows - 9), (0, 0)))
    length_block = jnp.broadcast_to(lengths.reshape(1, 1), (8, 128))
    (
        seq_rows, seq_seed, all_vec,
        query_full, key_full, value_full, out_full, inner_full, outer_full,
        query_rows, key_rows, value_rows, probs, context, first_normed, first_inv, hidden_low,
        activated, slope, second_normed, second_inv, result, kept_table, _,
    ) = fetch(
        rep_size, fsdp_size, slot_seq, tokens, cotangent, length_block, vec,
        [query_weight, key_weight, value_weight, out_weight, inner_weight, outer_weight],
    )
    back_rows, back_grads, (
        d_outer, d_inner, d_out, d_query, d_key, d_value, d_vec,
    ) = backward(
        rep_size, fsdp_size, result, probs,
        [
            outer_full, inner_full, out_full, query_full, key_full, value_full,
            seq_rows, seq_seed, query_rows, key_rows, value_rows, context,
            first_normed, second_normed, hidden_low, activated, slope,
        ],
        first_inv, second_inv, kept_table, all_vec,
    )
    d_outer, d_inner, d_out, d_query, d_key, d_value = widen(
        [d_outer, d_inner, d_out, d_query, d_key, d_value]
    )
    v = d_vec[:, :width]
    return (
        back_rows, back_grads,
        d_query, v[0], d_key, d_value, v[1], d_out, v[2], v[3], v[4],
        d_inner, d_vec[8 : 8 + inner_bias.shape[0] // 128, :128].reshape(-1), d_outer, v[5], v[6], v[7],
    )


def solution(mesh):
    placed = (
        P(("rep", "fsdp"), None),
        P(("rep", "fsdp"), None),
        P(("rep", "fsdp")),
        P(),
        P("fsdp", None),
        P("fsdp"),
        P("fsdp", None),
        P("fsdp", None),
        P("fsdp"),
        P("fsdp", None),
        P("fsdp"),
        P("fsdp"),
        P("fsdp"),
        P("fsdp", None),
        P("fsdp"),
        P("fsdp", None),
        P("fsdp"),
        P("fsdp"),
        P("fsdp"),
    )
    return jax.shard_map(
        shards,
        mesh=mesh,
        in_specs=placed,
        out_specs=(
            P(("rep", "fsdp"), None),
            P(("rep", "fsdp"), None),
            P("fsdp", None),
            P("fsdp"),
            P("fsdp", None),
            P("fsdp", None),
            P("fsdp"),
            P("fsdp", None),
            P("fsdp"),
            P("fsdp"),
            P("fsdp"),
            P("fsdp", None),
            P("fsdp"),
            P("fsdp", None),
            P("fsdp"),
            P("fsdp"),
            P("fsdp"),
        ),
        check_vma=False,
    )
```
